256 devices in a mesh: row: 8 (over x, core), col: 32 (over y, z).
Axes of the slice: x: 4, y: 4, z: 8, core: 2. Of those that a mesh axis runs over, the one named last changes fastest.
Arguments:
- pooled: bfloat16 [16384, 1152], P(('row', 'col')), may hold values from -32 to 32
- hidden: bfloat16 [16384, 4304], P(('row', 'col')), may hold values from -6 to 6
- text: bfloat16 [16384, 1152], P(('row', 'col')), may hold values from -12 to 12
- weight: float32 [1152, 4304], P('col', 'row'), may hold values from -0.09375 to 0.09375
- row_moment: float32 [1152], P('col'), may hold values from 1e-07 to 1e-05
- col_moment: float32 [4304], P('row'), may hold values from 1e-07 to 1e-05
- log_scale: float32 [], replicated, may hold values from 4.2 to 4.8
- bias: float32 [], replicated, may hold values from -16 to -12
Outputs:
- update: float32 [1152, 4304], P('col', 'row')
- new_row: float32 [1152], P('col')
- new_col: float32 [4304], P('row')
- loss: float32 [], replicated
The draws below stay inside these ranges and needn't reach their ends.
All inputs are finite; a program needn't handle non-finite values.
Results may differ from the reference program's by a relative error of at most 0.004.
Values may be sent and summed in bfloat16 or wider, within the bound.
No kernel may reach another device: no remote copies, remote signals or barrier semaphores. Data moves between devices by JAX's collectives and lax.ppermute only.
A program may use at most 128 MiB of HBM per device.

```python
import math
import jax
import jax.numpy as jnp
from jax import lax

D = 1152
FF = 4304
TOK_DEV = 64
BATCH = 16384
N_ROW = 8
N_COL = 32


def noise_block(key, shape):
    return jax.random.normal(key, shape, jnp.float32)


def pair_parts(key):
    folded = jax.random.fold_in(key, 4242)
    subkeys = jax.random.split(folded, 6)
    group_count = 16
    centers = noise_block(subkeys[0], (group_count, D))
    members = jax.random.randint(subkeys[1], (BATCH,), 0, group_count)
    onehot = (members[:, None] == jnp.arange(group_count, dtype=jnp.int32)[None, :]).astype(jnp.float32)
    cluster = jnp.dot(onehot, centers, precision=lax.Precision.HIGHEST)
    shared = noise_block(subkeys[2], (BATCH, D))
    strength = jax.random.uniform(subkeys[3], (BATCH, 1), jnp.float32, 0.1, 0.5)
    own_image = noise_block(subkeys[4], (BATCH, D))
    own_text = noise_block(subkeys[5], (BATCH, D))
    cluster_weight = 0.5
    image_side = cluster_weight * cluster + shared + 1.5 * own_image
    text_side = cluster_weight * cluster + strength * shared + 1.5 * own_text
    return (jnp.clip(image_side, -32.0, 32.0), jnp.clip(text_side, -12.0, 12.0))


def draw_pooled(key, part):
    return pair_parts(key)[0].astype(jnp.bfloat16)


def draw_text(key, part):
    return pair_parts(key)[1].astype(jnp.bfloat16)


def block_levels(key, extent, cuts, least, largest):
    loudness, own = 1.0, jax.random.fold_in(key, 6)
    for axis_at, shards_of in cuts:
        heights = jnp.exp(jax.random.uniform(jax.random.fold_in(own, axis_at), (shards_of,), jnp.float32, least / len(cuts), largest / len(cuts)))
        loudness = loudness * jnp.repeat(heights, extent[axis_at] // shards_of).reshape([-1 if axis == axis_at else 1 for axis in range(len(extent))])
    return loudness


def scatter_about(key, shape, spread, bound, cuts=(), kind=jnp.bfloat16):
    array = jax.random.normal(key, shape, jnp.float32) * spread
    if len(cuts) > 0:
        array = block_levels(key, shape, cuts, -0.22, 0.18) * array
    return jnp.clip(array, min=-bound, max=bound).astype(kind)


def setup_inputs(seed: int = 0) -> dict:
    streams_of = jax.random.split(jax.random.key(seed), 9)
    pooled = draw_pooled(jax.random.fold_in(streams_of[8], 71), 0)
    hidden = scatter_about(streams_of[1], (BATCH, FF), 1.0, 6.0, ((0, 256),))
    text = draw_text(jax.random.fold_in(streams_of[8], 71), 0)
    weight = scatter_about(streams_of[3], (D, FF), FF ** -0.5, 0.09375, ((0, 32), (1, 8)), jnp.float32)
    row_moment = jnp.clip(jnp.exp(math.log(9.999999747378752e-06) - 4.6051701 * jax.random.uniform(streams_of[4], (D,), jnp.float32) ** block_levels(streams_of[4], (D,), ((0, 32),), -0.2, 0.2)), 1.0000000116860974e-07, 9.999999747378752e-06)
    col_moment = jnp.clip(jnp.exp(math.log(9.999999747378752e-06) - 4.6051701 * jax.random.uniform(streams_of[5], (FF,), jnp.float32) ** block_levels(streams_of[5], (FF,), ((0, 8),), -0.2, 0.2)), 1.0000000116860974e-07, 9.999999747378752e-06)
    log_scale = jnp.clip(jax.random.uniform(streams_of[6], (), jnp.float32, 4.2, 4.8), 4.2, 4.8)
    bias = jnp.clip(jax.random.uniform(streams_of[7], (), jnp.float32, -16.0, -12.0), -16.0, -12.0)
    return dict(pooled=pooled, hidden=hidden, text=text, weight=weight, row_moment=row_moment, col_moment=col_moment, log_scale=log_scale, bias=bias)


EPSILON = 1e-06
DECAY_RATE = 0.8
CLIP_LEVEL = 1.0
FLOOR_VALUE = 1e-30

def reference(pooled, hidden, text, weight, row_moment, col_moment, log_scale, bias):
    batch_total = TOK_DEV * N_ROW * N_COL
    weight_half = weight.astype(jnp.bfloat16)
    projected = jnp.dot(hidden, weight_half.T, preferred_element_type=jnp.float32)
    mixed_rows = pooled.astype(jnp.float32) + projected
    length = jnp.sqrt(lax.optimization_barrier(jnp.sum(mixed_rows * mixed_rows, axis=1, keepdims=True)) + EPSILON)
    image_unit = mixed_rows / length
    images = image_unit.astype(jnp.bfloat16)
    text_float = text.astype(jnp.float32)
    text_units = (text_float / jnp.sqrt(lax.optimization_barrier(jnp.sum(text_float * text_float, axis=1, keepdims=True)) + EPSILON)).astype(jnp.bfloat16)
    logit_scale = jnp.exp(log_scale.astype(jnp.float32))
    block_rows = batch_total // N_ROW
    image_blocks = images.reshape(N_ROW, block_rows, D)
    text_ids = jnp.arange(batch_total, dtype=jnp.int32)

    def one_block(block_item):
        image_block, block_index = block_item
        image_ids = block_index * block_rows + jnp.arange(block_rows, dtype=jnp.int32)
        logits = logit_scale * jnp.dot(image_block, text_units.T, preferred_element_type=jnp.float32) + bias
        label_sign = jnp.where(image_ids[:, None] == text_ids[None, :], jnp.float32(1.0), jnp.float32(-1.0))
        loss_sum = jnp.sum(jax.nn.softplus(-label_sign * logits))
        grad_logits = (-label_sign * jax.nn.sigmoid(-label_sign * logits) / batch_total).astype(jnp.bfloat16)
        return (loss_sum, logit_scale * jnp.dot(grad_logits, text_units, preferred_element_type=jnp.float32))
    loss_sums, unit_grads = lax.map(one_block, (image_blocks, jnp.arange(N_ROW, dtype=jnp.int32)))
    loss = jnp.sum(loss_sums) / batch_total
    unit_grad = unit_grads.reshape(batch_total, D)
    mixed_grad = ((unit_grad - image_unit * lax.optimization_barrier(jnp.sum(image_unit * unit_grad, axis=1, keepdims=True))) / length).astype(jnp.bfloat16)
    gradient = jnp.dot(mixed_grad.T, hidden, preferred_element_type=jnp.float32)
    squared = gradient * gradient + FLOOR_VALUE
    new_row = DECAY_RATE * row_moment + (1.0 - DECAY_RATE) * lax.optimization_barrier(jnp.mean(squared, axis=1))
    new_col = DECAY_RATE * col_moment + (1.0 - DECAY_RATE) * lax.optimization_barrier(jnp.mean(squared, axis=0))
    second = new_row[:, None] * new_col[None, :]
    raw_update = gradient / jnp.sqrt(second)
    update_rms = jnp.sqrt(jnp.mean(raw_update * raw_update))
    update = raw_update / jnp.maximum(1.0, update_rms / CLIP_LEVEL)
    return (update, new_row, new_col, loss)
```

```python
import itertools

import jax
import jax.numpy as jnp
from jax import lax
from jax.sharding import Mesh
from jax.sharding import PartitionSpec as P

D = 1152
FF = 4304
AXES = ("x", "k", "y", "z")
SIZES = {"x": 4, "k": 2, "y": 4, "z": 8}
ROW = ("x", "k")
COL = ("y", "z")
EPSILON = 1e-06
DECAY_RATE = 0.8
CLIP_LEVEL = 1.0
FLOOR_VALUE = 1e-30
BF16 = jnp.bfloat16
F32 = jnp.float32


def shift(value, **by):
    names = tuple(a for a in AXES if a in by)
    sizes = [SIZES[a] for a in names]

    def linear(place):
        index = 0
        for p, n in zip(place, sizes):
            index = index * n + p
        return index

    pairs = [
        (linear(p), linear([(c + by[a]) % SIZES[a] for c, a in zip(p, names)]))
        for p in itertools.product(*[range(n) for n in sizes])
    ]
    return lax.ppermute(value, names, pairs)


def exchange(pieces, axes):
    return lax.all_to_all(pieces, axes, split_axis=0, concat_axis=0, tiled=True)


def everywhere(array, axes):
    return exchange(jnp.broadcast_to(array, (lax.axis_size(axes), *array.shape)), axes)


def pair_tile(images, texts, positive, logit_scale, bias, batch_total):
    logits = (
        logit_scale
        * lax.dot_general(images, texts, (((1,), (1,)), ((), ())), preferred_element_type=F32)
        + bias
    )
    if positive is None:
        turned = logits
        sign = F32(1.0)
    else:
        turned = jnp.where(positive, -logits, logits)
        sign = jnp.where(positive, F32(-1.0), F32(1.0))
    loss_sum = jnp.sum(jax.nn.softplus(turned))
    grads = (sign * jax.nn.sigmoid(turned) / batch_total).astype(BF16)
    return loss_sum, jnp.dot(grads, texts, preferred_element_type=F32)


def per_device(pooled, hidden, text, weight, row_moment, col_moment, log_scale, bias):
    tokens = pooled.shape[0]
    batch_total = tokens * 256
    slice_ff = weight.shape[1]
    x_place = lax.axis_index("x")
    k_place = lax.axis_index("k")
    col_place = lax.axis_index(COL)

    text_float = text.astype(F32)
    text_units = (
        text_float / jnp.sqrt(jnp.sum(text_float * text_float, axis=1, keepdims=True) + EPSILON)
    ).astype(BF16)
    texts_own = lax.all_gather(text_units, COL, axis=0, tiled=True)

    hidden_x = exchange(
        jnp.moveaxis(hidden.reshape(tokens, 4, 2 * slice_ff), 1, 0), "x"
    )
    weight_own = everywhere(weight.astype(BF16), COL).reshape(D, slice_ff)
    weight_other = shift(weight_own, k=1)
    low, high = hidden_x[..., :slice_ff], hidden_x[..., slice_ff:]
    first_core = k_place == 0
    hid_own = jnp.where(first_core, low, high)
    hid_other = jnp.where(first_core, high, low)
    contract = (((2,), (1,)), ((), ()))
    partial = lax.dot_general(
        hid_own, weight_own, contract, preferred_element_type=F32
    ) + lax.dot_general(hid_other, weight_other, contract, preferred_element_type=F32)
    arrived = exchange(partial.astype(BF16), "x")
    mixed = pooled.astype(F32) + jnp.sum(arrived.astype(F32), axis=0)
    length = jnp.sqrt(jnp.sum(mixed * mixed, axis=1, keepdims=True) + EPSILON)
    unit = mixed / length
    images = unit.astype(BF16)

    hid_pair, _ = lax.optimization_barrier((jnp.stack([hid_own, hid_other]), weight_own))
    hid_y = [hid_pair] + [shift(hid_pair, y=s) for s in (1, 2, 3)]

    texts_other = shift(texts_own, k=1)
    logit_scale = jnp.exp(log_scale)
    image_rows = jnp.concatenate([images] + [shift(images, x=s) for s in (1, 2, 3)])
    rows = lax.broadcasted_iota(jnp.int32, (4 * tokens, texts_own.shape[0]), 0)
    cols = lax.broadcasted_iota(jnp.int32, (4 * tokens, texts_own.shape[0]), 1)
    positive = (rows < tokens) & (cols == rows + col_place * tokens)
    loss_a, part_a = pair_tile(image_rows, texts_own, positive, logit_scale, bias, batch_total)
    loss_b, part_b = pair_tile(image_rows, texts_other, None, logit_scale, bias, batch_total)
    unit_part = (logit_scale * (part_a + part_b)).reshape(4, tokens, D)
    unit_send = unit_part.astype(BF16)
    unit_grad = unit_part[0] + sum(shift(unit_send[s], x=-s).astype(F32) for s in (1, 2, 3))
    mixed_grad = (
        (unit_grad - unit * jnp.sum(unit * unit_grad, axis=1, keepdims=True)) / length
    ).astype(BF16)

    quarters = jnp.moveaxis(mixed_grad.reshape(tokens, 4, D // 4), 1, 0)
    grad_rows = exchange(
        jnp.broadcast_to(quarters[None], (4, 4, tokens, D // 4)).reshape(16, tokens, D // 4),
        ("x", "y"),
    ).reshape(4, 4, tokens, D // 4)
    y_place = lax.axis_index("y")
    grad_by_y = jnp.moveaxis(grad_rows, 1, 0)
    both = [F32(0.0), F32(0.0)]
    for s in range(4):
        part = lax.dynamic_index_in_dim(grad_by_y, (y_place - s) % 4, 0, keepdims=False)
        part = part.reshape(4 * tokens, D // 4)
        for which in range(2):
            both[which] = both[which] + lax.dot_general(
                part,
                hid_y[s][which].reshape(4 * tokens, slice_ff),
                (((0,), (0,)), ((), ())),
                preferred_element_type=F32,
            )
    chip_grad = both[0] + shift(both[1], k=1)
    arrived_grad = exchange(chip_grad.astype(BF16).reshape(8, D // 32, slice_ff), "z")
    gradient = jnp.sum(arrived_grad.astype(F32), axis=0)

    squared = gradient * gradient + FLOOR_VALUE
    row_message = jnp.concatenate([jnp.sum(squared, axis=1), (loss_a + loss_b).reshape(1)])
    row_total = jnp.sum(everywhere(row_message[None], ROW), axis=(0, 1))
    loss_row = row_total[-1]
    new_row = DECAY_RATE * row_moment + (1.0 - DECAY_RATE) * row_total[:-1] / FF
    scaled = jnp.sum(gradient * gradient / new_row[:, None], axis=0)
    col_message = jnp.stack(
        [jnp.sum(squared, axis=0), scaled, jnp.full((slice_ff,), loss_row)]
    )
    col_total = jnp.sum(everywhere(col_message, COL), axis=0)
    new_col = DECAY_RATE * col_moment + (1.0 - DECAY_RATE) * col_total[0] / D
    loss = col_total[2, 0] / batch_total
    ours = jnp.sum(col_total[1] / new_col)
    update_total = jnp.sum(everywhere(jnp.full((1, 128), ours), ROW), axis=(0, 1))[0]
    update_rms = jnp.sqrt(update_total / (D * FF))
    raw_update = gradient / jnp.sqrt(new_row[:, None] * new_col[None, :])
    update = raw_update / jnp.maximum(1.0, update_rms / CLIP_LEVEL)
    return (update, new_row, new_col, loss)


def solution(mesh):
    finer = Mesh(mesh.devices.reshape(4, 2, 4, 8), AXES)
    return jax.shard_map(
        per_device,
        mesh=finer,
        in_specs=(
            P(AXES, None),
            P(AXES, None),
            P(AXES, None),
            P(COL, ROW),
            P(COL),
            P(ROW),
            P(),
            P(),
        ),
        out_specs=(P(COL, ROW), P(COL), P(ROW), P()),
        check_vma=False,
    )
```

```python
import itertools

import jax
import jax.numpy as jnp
from jax import lax
from jax.sharding import Mesh
from jax.sharding import PartitionSpec as P

D = 1152
FF = 4304
AXES = ("x", "k", "y", "z")
SIZES = {"x": 4, "k": 2, "y": 4, "z": 8}
ROW = ("x", "k")
COL = ("y", "z")
EPSILON = 1e-06
DECAY_RATE = 0.8
CLIP_LEVEL = 1.0
FLOOR_VALUE = 1e-30
BF16 = jnp.bfloat16
F32 = jnp.float32


def shift(value, **by):
    names = tuple(a for a in AXES if a in by)
    sizes = [SIZES[a] for a in names]

    def linear(place):
        index = 0
        for p, n in zip(place, sizes):
            index = index * n + p
        return index

    pairs = [
        (linear(p), linear([(c + by[a]) % SIZES[a] for c, a in zip(p, names)]))
        for p in itertools.product(*[range(n) for n in sizes])
    ]
    return lax.ppermute(value, names, pairs)


def exchange(pieces, axes):
    return lax.all_to_all(pieces, axes, split_axis=0, concat_axis=0, tiled=True)


def everywhere(array, axes):
    return exchange(jnp.broadcast_to(array, (lax.axis_size(axes), *array.shape)), axes)


def after(values, *others):
    return lax.optimization_barrier((values, others))[0]


def ring_step(up, down, axis):
    return shift(up, **{axis: 1}), shift(down, **{axis: -1})


def pair_tile(images, texts, positive, logit_scale, bias, batch_total):
    logits = (
        logit_scale
        * lax.dot_general(images, texts, (((1,), (1,)), ((), ())), preferred_element_type=F32)
        + bias
    )
    if positive is None:
        turned = logits
        sign = F32(1.0)
    else:
        turned = jnp.where(positive, -logits, logits)
        sign = jnp.where(positive, F32(-1.0), F32(1.0))
    loss_sum = jnp.sum(jax.nn.softplus(turned))
    grads = (sign * jax.nn.sigmoid(turned) / batch_total).astype(BF16)
    return loss_sum, jnp.dot(grads, texts, preferred_element_type=F32)


def per_device(pooled, hidden, text, weight, row_moment, col_moment, log_scale, bias):
    tokens = pooled.shape[0]
    batch_total = tokens * 256
    slice_ff = weight.shape[1]
    k_place = lax.axis_index("k")

    first_core = k_place == 0
    quarter = D // 4
    hidden_x = exchange(
        jnp.moveaxis(hidden.reshape(tokens, 4, 2 * slice_ff), 1, 0), "x"
    ).reshape(4 * tokens, 2 * slice_ff)
    hid_y = [hidden_x] + [shift(hidden_x, y=-s) for s in (1, 2, 3)]

    text_float = text.astype(F32)
    text_units = (
        text_float / jnp.sqrt(jnp.sum(text_float * text_float, axis=1, keepdims=True) + EPSILON)
    ).astype(BF16)
    texts_y = jnp.concatenate([text_units] + [shift(text_units, k=1, y=s) for s in (1, 2, 3)])
    up, down = ring_step(texts_y, texts_y, "z")
    ring_pieces = [texts_y, up, down]

    weight_own = everywhere(after(weight.astype(BF16), texts_y, hidden_x), "z").reshape(quarter, slice_ff)
    weight_other = shift(weight_own, k=1)
    weight_x = jnp.concatenate(
        [
            jnp.where(first_core, weight_own, weight_other),
            jnp.where(first_core, weight_other, weight_own),
        ],
        axis=1,
    )
    partial = jnp.stack(
        [
            lax.dot_general(
                piece, weight_x, (((1,), (1,)), ((), ())), preferred_element_type=F32
            )
            .astype(BF16)
            .reshape(4, tokens, quarter)
            for piece in hid_y
        ]
    )
    y_place = lax.axis_index("y")
    partial = jnp.stack(
        [
            lax.dynamic_index_in_dim(partial, (c - y_place) & 3, 0, keepdims=False)
            for c in range(4)
        ],
        axis=1,
    )
    arrived = exchange(after(partial.reshape(16, tokens, quarter), up, down), ("x", "y"))
    half = texts_y.shape[0] // 2
    up, down = ring_step(up, down, "z")
    ring_pieces += [up, down]
    arrived = after(arrived, up, down)
    up, down = ring_step(up, down, "z")
    ring_pieces += [up, down]
    projected = jnp.sum(arrived.astype(F32).reshape(4, 4, tokens, quarter), axis=0)
    mixed = pooled.astype(F32) + jnp.moveaxis(projected, 0, 1).reshape(tokens, D)
    length = jnp.sqrt(jnp.sum(mixed * mixed, axis=1, keepdims=True) + EPSILON)
    unit = mixed / length
    images = after(unit.astype(BF16), up, down)
    ring_pieces += ring_step(up[:half], down[half:], "z")

    logit_scale = jnp.exp(log_scale)
    image_rows = jnp.concatenate([images] + [shift(images, x=s) for s in (1, 2, 3)])
    texts_own = jnp.concatenate(ring_pieces[:-2] + after(ring_pieces[-2:], image_rows))
    texts_other = shift(texts_own, k=1)
    rows = lax.broadcasted_iota(jnp.int32, (4 * tokens, texts_own.shape[0]), 0)
    cols = lax.broadcasted_iota(jnp.int32, (4 * tokens, texts_own.shape[0]), 1)
    positive = (rows < tokens) & (cols == rows)
    loss_a, part_a = pair_tile(image_rows, texts_own, positive, logit_scale, bias, batch_total)
    loss_b, part_b = pair_tile(image_rows, texts_other, None, logit_scale, bias, batch_total)
    unit_part = (logit_scale * (part_a + part_b)).reshape(4, tokens, D)
    unit_send = unit_part.astype(BF16)
    unit_grad = unit_part[0] + sum(shift(unit_send[s], x=-s).astype(F32) for s in (1, 2, 3))
    mixed_grad = (
        (unit_grad - unit * jnp.sum(unit * unit_grad, axis=1, keepdims=True)) / length
    ).astype(BF16)

    quarters = jnp.moveaxis(mixed_grad.reshape(tokens, 4, quarter), 1, 0)
    grad_rows = exchange(
        jnp.broadcast_to(quarters[None], (4, 4, tokens, quarter)).reshape(16, tokens, quarter),
        ("x", "y"),
    ).reshape(4, 4, tokens, quarter)
    grad_by_y = jnp.moveaxis(grad_rows, 1, 0).reshape(4, 4 * tokens, quarter)
    both = F32(0.0)
    for s in range(4):
        part = lax.dynamic_index_in_dim(grad_by_y, (y_place + s) & 3, 0, keepdims=False)
        both = both + lax.dot_general(
            part, hid_y[s], (((0,), (0,)), ((), ())), preferred_element_type=F32
        )
    low, high = both[:, :slice_ff], both[:, slice_ff:]
    chip_grad = jnp.where(first_core, low, high) + shift(jnp.where(first_core, high, low), k=1)
    arrived_grad = exchange(chip_grad.astype(BF16).reshape(8, D // 32, slice_ff), "z")
    gradient = jnp.sum(arrived_grad.astype(F32), axis=0)

    squared = gradient * gradient + FLOOR_VALUE
    row_message = jnp.concatenate([jnp.sum(squared, axis=1), (loss_a + loss_b).reshape(1)])
    row_total = jnp.sum(everywhere(row_message[None], ROW), axis=(0, 1))
    loss_row = row_total[-1]
    new_row = DECAY_RATE * row_moment + (1.0 - DECAY_RATE) * row_total[:-1] / FF
    scaled = jnp.sum(gradient * gradient / new_row[:, None], axis=0)
    col_message = jnp.stack(
        [jnp.sum(squared, axis=0), scaled, jnp.full((slice_ff,), loss_row)]
    )
    col_total = jnp.sum(everywhere(col_message, COL), axis=0)
    new_col = DECAY_RATE * col_moment + (1.0 - DECAY_RATE) * col_total[0] / D
    loss = col_total[2, 0] / batch_total
    ours = jnp.sum(col_total[1] / new_col)
    update_total = jnp.sum(everywhere(jnp.full((1, 128), ours), ROW), axis=(0, 1))[0]
    update_rms = jnp.sqrt(update_total / (D * FF))
    raw_update = gradient / jnp.sqrt(new_row[:, None] * new_col[None, :])
    update = raw_update / jnp.maximum(1.0, update_rms / CLIP_LEVEL)
    return (update, new_row, new_col, loss)


def solution(mesh):
    finer = Mesh(mesh.devices.reshape(4, 2, 4, 8), AXES)
    return jax.shard_map(
        per_device,
        mesh=finer,
        in_specs=(
            P(AXES, None),
            P(AXES, None),
            P(AXES, None),
            P(COL, ROW),
            P(COL),
            P(ROW),
            P(),
            P(),
        ),
        out_specs=(P(COL, ROW), P(COL), P(ROW), P()),
        check_vma=False,
    )
```

```python
import functools
import itertools

import jax
import jax.numpy as jnp
from jax import lax
from jax.experimental import pallas as pl
from jax.experimental.pallas import tpu as pltpu
from jax.sharding import Mesh
from jax.sharding import PartitionSpec as P


D = 1152
FF = 4304
AXES = ("x", "k", "y", "z")
SIZES = {"x": 4, "k": 2, "y": 4, "z": 8}
ROW = ("x", "k")
COL = ("y", "z")
EPSILON = 1e-06
DECAY_RATE = 0.8
CLIP_LEVEL = 1.0
FLOOR_VALUE = 1e-30
BF16 = jnp.bfloat16
F32 = jnp.float32


def shift(value, **by):
    names = tuple(a for a in AXES if a in by)
    sizes = [SIZES[a] for a in names]

    def linear(place):
        index = 0
        for p, n in zip(place, sizes):
            index = index * n + p
        return index

    pairs = [
        (linear(p), linear([(c + by[a]) % SIZES[a] for c, a in zip(p, names)]))
        for p in itertools.product(*[range(n) for n in sizes])
    ]
    return lax.ppermute(value, names, pairs)


def exchange(pieces, axes):
    return lax.all_to_all(pieces, axes, split_axis=0, concat_axis=0, tiled=True)


def everywhere(array, axes):
    return exchange(jnp.broadcast_to(array, (lax.axis_size(axes), *array.shape)), axes)


def after(values, *others):
    return lax.optimization_barrier((values, others))[0]


def rolled(pieces, by, count):
    twice = jnp.concatenate([pieces, pieces])
    return lax.dynamic_slice_in_dim(twice, by & (count - 1), count, 0)


def ring_step(up, down, axis):
    return shift(up, **{axis: 1}), shift(down, **{axis: -1})


def project_kernel(h0, h1, h2, h3, own, other, part, *hid):
    at = pl.program_id(0)
    total = None
    for kk in range(2):
        rows = jnp.concatenate([h[0, kk] for h in (h0, h1, h2, h3)], axis=0)
        for s in range(4):

            @pl.when(at == s)
            def _(s=s, rows=rows):
                hid[s][kk] = rows

        piece = lax.dot_general(
            rows, (own, other)[kk][0], (((1,), (1,)), ((), ())), preferred_element_type=F32
        )
        total = piece if total is None else total + piece

    @pl.when(at == 0)
    def _():
        part[...] = total

    @pl.when(at > 0)
    def _():
        part[...] += total


def project(hid_y, own, other):
    count, _, tokens, units = hid_y[0].shape
    features = own.shape[1]
    weights = pl.BlockSpec((1, features, units), lambda i: (i, 0, 0))
    rows = (2, 4 * tokens, units)
    return pl.pallas_call(
        project_kernel,
        grid=(count,),
        in_specs=[pl.BlockSpec((1, 2, tokens, units), lambda i: (i, 0, 0, 0))] * 4
        + [weights] * 2,
        out_specs=[pl.BlockSpec((4 * tokens, features), lambda i: (0, 0))]
        + [pl.BlockSpec(rows, lambda i: (0, 0, 0))] * 4,
        out_shape=[jax.ShapeDtypeStruct((4 * tokens, features), F32)]
        + [jax.ShapeDtypeStruct(rows, BF16)] * 4,
        cost_estimate=pl.CostEstimate(
            flops=2 * count * 2 * 4 * tokens * units * features,
            bytes_accessed=8000000,
            transcendentals=0,
        ),
        compiler_params=pltpu.CompilerParams(dimension_semantics=("arbitrary",)),
    )(*hid_y, own, other)


def gradient_kernel(*refs):
    grads, hid, outs = refs[:4], refs[4:8], refs[8:]
    totals = [None, None]
    for s in range(4):
        turned = grads[s][...].T
        for kk in range(2):
            piece = jnp.dot(
                turned, hid[s][kk if s == 0 else 1 - kk], preferred_element_type=F32
            )
            totals[kk] = piece if totals[kk] is None else totals[kk] + piece
    for kk in range(2):
        outs[kk][...] = totals[kk]


def gradients(grads, hid):
    features, units = grads[0].shape[1], hid[0].shape[2]
    return pl.pallas_call(
        gradient_kernel,
        out_shape=[jax.ShapeDtypeStruct((features, units), F32)] * 2,
        cost_estimate=pl.CostEstimate(
            flops=16 * grads[0].size * units, bytes_accessed=4000000, transcendentals=0
        ),
    )(*grads, *hid)


def joined(pieces):
    rows = sum(p.shape[0] for p in pieces)
    whole = jnp.zeros((rows, *pieces[0].shape[1:]), pieces[0].dtype)
    at = 0
    for piece in pieces:
        whole = lax.dynamic_update_slice_in_dim(whole, piece, at, 0)
        at += piece.shape[0]
    return whole


def pair_kernel(scalars, images, texts, *refs, first, tokens, batch_total):
    if first:
        part, loss = refs
    else:
        before, part, sent, loss = refs
    at = pl.program_id(0)
    block = texts[...]
    logits = (
        scalars[0]
        * lax.dot_general(
            images[...], block, (((1,), (1,)), ((), ())), preferred_element_type=F32
        )
        + scalars[1]
    )
    if first:
        rows = lax.broadcasted_iota(jnp.int32, logits.shape, 0)
        cols = lax.broadcasted_iota(jnp.int32, logits.shape, 1) + at * logits.shape[1]
        positive = (rows == cols) & (rows < tokens)
        logits = jnp.where(positive, -logits, logits)
    small = jnp.exp(-jnp.abs(logits))
    inverse = 1.0 / (1.0 + small)
    slope = jnp.where(logits >= 0, inverse, small * inverse) / batch_total
    if first:
        slope = jnp.where(positive, -slope, slope)
    added = jnp.dot(slope.astype(BF16), block, preferred_element_type=F32)
    losses = jnp.sum(jnp.maximum(logits, 0.0) + jnp.log1p(small), axis=0, keepdims=True)

    @pl.when(at == 0)
    def _():
        loss[...] = losses
        part[...] = added if first else added + before[...]

    @pl.when(at > 0)
    def _():
        loss[...] += losses
        part[...] += added

    if not first:

        @pl.when(at == pl.num_programs(0) - 1)
        def _():
            scaled = scalars[0] * part[...]
            part[...] = scaled
            sent[...] = scaled.astype(BF16)


def pair_tiles(scalars, images, texts, before, tokens, batch_total):
    first = before is None
    count, width = images.shape
    block = 256
    whole = pl.BlockSpec((count, width), lambda i: (0, 0))
    outs = [jax.ShapeDtypeStruct((count, width), F32)]
    if not first:
        outs.append(jax.ShapeDtypeStruct((count, width), BF16))
    outs.append(jax.ShapeDtypeStruct((1, block), F32))
    pairs = count * texts.shape[0]
    return pl.pallas_call(
        functools.partial(
            pair_kernel, first=first, tokens=tokens, batch_total=batch_total
        ),
        grid=(texts.shape[0] // block,),
        in_specs=[
            pl.BlockSpec(memory_space=pltpu.SMEM),
            whole,
            pl.BlockSpec((block, width), lambda i: (i, 0)),
        ]
        + ([] if first else [whole]),
        out_specs=[whole] * (len(outs) - 1) + [pl.BlockSpec((1, block), lambda i: (0, 0))],
        out_shape=outs,
        cost_estimate=pl.CostEstimate(
            flops=4 * pairs * width, bytes_accessed=2 * texts.size, transcendentals=3 * pairs
        ),
        compiler_params=pltpu.CompilerParams(dimension_semantics=("arbitrary",)),
    )(scalars, images, texts, *([] if first else [before]))


def step(pooled, hidden, text, weight, row_moment, col_moment, log_scale, bias):
    tokens = pooled.shape[0]
    batch_total = tokens * 256
    slice_ff = weight.shape[1]
    k_place = lax.axis_index("k")

    quarter = D // 4
    x_place = lax.axis_index("x")
    y_place = lax.axis_index("y")
    half_ff = slice_ff

    text_float = text.astype(F32)
    text_units = (
        text_float / jnp.sqrt(jnp.sum(text_float * text_float, axis=1, keepdims=True) + EPSILON)
    ).astype(BF16)
    texts_y = joined([text_units] + [shift(text_units, k=1, y=s) for s in (1, 2, 3)])

    by_slice = jnp.moveaxis(hidden.reshape(tokens, 8, half_ff), 1, 0).reshape(
        4, 2, tokens, half_ff
    )
    by_slice = jnp.where(k_place == 0, by_slice, by_slice[:, ::-1])
    hid_mine = rolled(by_slice, x_place, 4)
    hid_y = [hid_mine] + [shift(hid_mine, y=-s) for s in (1, 2, 3)]

    up, down = ring_step(texts_y, texts_y, "z")
    ring_pieces = [texts_y, up, down]

    weight_z = everywhere(weight.astype(BF16), "z").reshape(quarter, half_ff)
    weight_own = [weight_z] + [shift(weight_z, x=-s) for s in (1, 2, 3)]
    weight_own = joined([w[None] for w in weight_own])
    weight_other = shift(after(weight_own, up, down), k=1)
    up, down = ring_step(up, down, "z")
    ring_pieces += [up, down]
    mixed_part, *hid_all = project(hid_y, weight_own, weight_other)
    mixed_part = mixed_part.reshape(4, tokens, quarter)

    by_y = (2, 4, tokens, half_ff)
    hid_x = [hid_all[0]] + [
        shift(hid_all[s].reshape(by_y), x=s, k=1).reshape(hid_all[s].shape)
        for s in (1, 2, 3)
    ]
    arrived = exchange(rolled(mixed_part, -y_place, 4), "y")
    mixed = pooled.astype(F32) + jnp.moveaxis(arrived, 0, 1).reshape(tokens, D)
    length = jnp.sqrt(jnp.sum(mixed * mixed, axis=1, keepdims=True) + EPSILON)
    unit = mixed / length
    images = unit.astype(BF16)
    up, down = ring_step(*after((up, down), mixed_part), "z")
    ring_pieces += [up, down]
    half = texts_y.shape[0] // 2
    ring_pieces += ring_step(*after((up[:half], down[half:]), images), "z")

    logit_scale = jnp.exp(log_scale)
    image_rows = joined([images] + [shift(images, x=s) for s in (1, 2, 3)])
    texts_own = jnp.concatenate(ring_pieces[:-2] + after(ring_pieces[-2:], image_rows))
    texts_other = shift(texts_own, k=1)
    scalars = jnp.stack([logit_scale, bias])
    part_a, loss_a = pair_tiles(scalars, image_rows, texts_own, None, tokens, batch_total)
    part, part_sent, loss_b = pair_tiles(
        scalars, image_rows, texts_other, part_a, tokens, batch_total
    )
    unit_grad = part[:tokens] + sum(
        shift(part_sent[s * tokens : (s + 1) * tokens], x=-s).astype(F32) for s in (1, 2, 3)
    )
    mixed_grad = (
        (unit_grad - unit * jnp.sum(unit * unit_grad, axis=1, keepdims=True)) / length
    ).astype(BF16)

    quarters = jnp.moveaxis(mixed_grad.reshape(tokens, 4, quarter), 1, 0)
    quarters = rolled(quarters, y_place, 4)
    grad_y = [quarters[0]] + [shift(quarters[s], y=s) for s in (1, 2, 3)]
    grad_mine = joined([grad_y[-s] for s in range(4)])
    grad_x = [grad_mine] + [shift(grad_mine, x=s, k=1) for s in (1, 2, 3)]
    both = gradients(grad_x, hid_x)
    chip_grad = both[0] + shift(both[1], k=1)
    arrived_grad = exchange(chip_grad.astype(BF16).reshape(8, D // 32, slice_ff), "z")
    gradient = jnp.sum(arrived_grad.astype(F32), axis=0)

    squared = gradient * gradient + FLOOR_VALUE
    row_message = jnp.concatenate([jnp.sum(squared, axis=1), jnp.sum(loss_a + loss_b).reshape(1)])
    row_total = jnp.sum(everywhere(row_message[None], ROW), axis=(0, 1))
    loss_row = row_total[-1]
    new_row = DECAY_RATE * row_moment + (1.0 - DECAY_RATE) * row_total[:-1] / FF
    scaled = jnp.sum(gradient * gradient / new_row[:, None], axis=0)
    col_message = jnp.stack(
        [jnp.sum(squared, axis=0), scaled, jnp.full((slice_ff,), loss_row)]
    )
    col_total = jnp.sum(everywhere(col_message, COL), axis=0)
    new_col = DECAY_RATE * col_moment + (1.0 - DECAY_RATE) * col_total[0] / D
    loss = col_total[2, 0] / batch_total
    ours = jnp.sum(col_total[1] / new_col)
    update_total = jnp.sum(everywhere(jnp.full((1, 128), ours), ROW), axis=(0, 1))[0]
    update_rms = jnp.sqrt(update_total / (D * FF))
    raw_update = gradient / jnp.sqrt(new_row[:, None] * new_col[None, :])
    update = raw_update / jnp.maximum(1.0, update_rms / CLIP_LEVEL)
    return (update, new_row, new_col, loss)


def solution(mesh):
    finer = Mesh(mesh.devices.reshape(4, 2, 4, 8), AXES)
    return jax.shard_map(
        step,
        mesh=finer,
        in_specs=(
            P(AXES, None),
            P(AXES, None),
            P(AXES, None),
            P(COL, ROW),
            P(COL),
            P(ROW),
            P(),
            P(),
        ),
        out_specs=(P(COL, ROW), P(COL), P(ROW), P()),
        check_vma=False,
    )
```

```python
import functools
import itertools

import jax
import jax.numpy as jnp
from jax import lax
from jax.experimental import pallas as pl
from jax.experimental.pallas import tpu as pltpu
from jax.sharding import Mesh
from jax.sharding import PartitionSpec as P


D = 1152
FF = 4304
AXES = ("x", "k", "y", "z")
SIZES = {"x": 4, "k": 2, "y": 4, "z": 8}
ROW = ("x", "k")
COL = ("y", "z")
EPSILON = 1e-06
DECAY_RATE = 0.8
CLIP_LEVEL = 1.0
FLOOR_VALUE = 1e-30
BF16 = jnp.bfloat16
F32 = jnp.float32


def shift(value, **by):
    names = tuple(a for a in AXES if a in by)
    sizes = [SIZES[a] for a in names]

    def linear(place):
        index = 0
        for p, n in zip(place, sizes):
            index = index * n + p
        return index

    pairs = [
        (linear(p), linear([(c + by[a]) % SIZES[a] for c, a in zip(p, names)]))
        for p in itertools.product(*[range(n) for n in sizes])
    ]
    return lax.ppermute(value, names, pairs)


def exchange(pieces, axes):
    return lax.all_to_all(pieces, axes, split_axis=0, concat_axis=0, tiled=True)


def everywhere(array, axes):
    return exchange(jnp.broadcast_to(array, (lax.axis_size(axes), *array.shape)), axes)


def after(values, *others):
    return lax.optimization_barrier((values, others))[0]


def rolled(pieces, by, count):
    twice = jnp.concatenate([pieces, pieces])
    return lax.dynamic_slice_in_dim(twice, by & (count - 1), count, 0)


def ring_step(up, down, axis):
    return shift(up, **{axis: 1}), shift(down, **{axis: -1})


def project_kernel(h0, h1, h2, h3, own, other, part, *hid):
    at = pl.program_id(0)
    total = None
    for kk in range(2):
        rows = jnp.concatenate([h[0, kk] for h in (h0, h1, h2, h3)], axis=0)
        for s in range(4):

            @pl.when(at == s)
            def _(s=s, rows=rows):
                hid[s][kk] = rows

        piece = lax.dot_general(
            rows, (own, other)[kk][0], (((1,), (1,)), ((), ())), preferred_element_type=F32
        )
        total = piece if total is None else total + piece

    @pl.when(at == 0)
    def _():
        part[...] = total

    @pl.when(at > 0)
    def _():
        part[...] += total


def project(hid_y, own, other):
    count, _, tokens, units = hid_y[0].shape
    features = own.shape[1]
    weights = pl.BlockSpec((1, features, units), lambda i: (i, 0, 0))
    rows = (2, 4 * tokens, units)
    return pl.pallas_call(
        project_kernel,
        grid=(count,),
        in_specs=[pl.BlockSpec((1, 2, tokens, units), lambda i: (i, 0, 0, 0))] * 4
        + [weights] * 2,
        out_specs=[pl.BlockSpec((4 * tokens, features), lambda i: (0, 0))]
        + [pl.BlockSpec(rows, lambda i: (0, 0, 0))] * 4,
        out_shape=[jax.ShapeDtypeStruct((4 * tokens, features), F32)]
        + [jax.ShapeDtypeStruct(rows, BF16)] * 4,
        cost_estimate=pl.CostEstimate(
            flops=2 * count * 2 * 4 * tokens * units * features,
            bytes_accessed=8000000,
            transcendentals=0,
        ),
        compiler_params=pltpu.CompilerParams(dimension_semantics=("arbitrary",)),
    )(*hid_y, own, other)


def gradient_kernel(*refs):
    grads, hid, outs = refs[:4], refs[4:8], refs[8:]
    total = None
    for s in range(4):
        piece = jnp.dot(grads[s][...].T, hid[s][0], preferred_element_type=F32)
        total = piece if total is None else total + piece
    for kk in range(2):

        @pl.when(pl.program_id(0) == kk)
        def _(kk=kk):
            outs[kk][...] = total


def gradients(grads, hid):
    tokens, features = grads[0].shape
    units = hid[0].shape[2]
    whole = pl.BlockSpec((features, units), lambda i: (0, 0))
    return pl.pallas_call(
        gradient_kernel,
        grid=(2,),
        in_specs=[pl.BlockSpec((tokens, features), lambda i: (0, 0))] * 4
        + [pl.BlockSpec((1, tokens, units), lambda i: (i, 0, 0))]
        + [pl.BlockSpec((1, tokens, units), lambda i: (1 - i, 0, 0))] * 3,
        out_specs=[whole] * 2,
        out_shape=[jax.ShapeDtypeStruct((features, units), F32)] * 2,
        cost_estimate=pl.CostEstimate(
            flops=16 * grads[0].size * units, bytes_accessed=4000000, transcendentals=0
        ),
        compiler_params=pltpu.CompilerParams(dimension_semantics=("arbitrary",)),
    )(*grads, *hid)


def joined(pieces):
    rows = sum(p.shape[0] for p in pieces)
    whole = jnp.zeros((rows, *pieces[0].shape[1:]), pieces[0].dtype)
    at = 0
    for piece in pieces:
        whole = lax.dynamic_update_slice_in_dim(whole, piece, at, 0)
        at += piece.shape[0]
    return whole


def pair_kernel(scalars, images, texts, *refs, first, tokens, batch_total, block):
    if first:
        part, loss, kept = refs
        part[...] = jnp.zeros(part.shape, F32)
    else:
        before, part, sent, loss, kept = refs
        part[...] = before[...]
    loss[...] = jnp.zeros(loss.shape, F32)
    count = texts.shape[0] // block

    def block_of(at):
        return texts[pl.ds(pl.multiple_of(at * block, block), block), :]

    def logits_of(at):
        return (
            scalars[0]
            * lax.dot_general(
                images[...], block_of(at), (((1,), (1,)), ((), ())), preferred_element_type=F32
            )
            + scalars[1]
        )

    kept[0] = logits_of(0)

    def one(at, _):
        logits = kept[at & 1]
        kept[(at + 1) & 1] = logits_of(jnp.minimum(at + 1, count - 1))
        if first:
            rows = lax.broadcasted_iota(jnp.int32, logits.shape, 0)
            cols = lax.broadcasted_iota(jnp.int32, logits.shape, 1) + at * block
            positive = (rows == cols) & (rows < tokens)
            logits = jnp.where(positive, -logits, logits)
        small = jnp.exp(-jnp.abs(logits))
        base = 1.0 + small
        inverse = 1.0 / base
        slope = jnp.where(logits >= 0, inverse, small * inverse) / batch_total
        if first:
            slope = jnp.where(positive, -slope, slope)
        part[...] += jnp.dot(
            slope.astype(BF16), block_of(at), preferred_element_type=F32
        )
        softplus = jnp.maximum(logits, 0.0) + (
            jnp.log(base) + (small - (base - 1.0)) * inverse
        )
        loss[...] += jnp.sum(softplus, axis=0, keepdims=True)
        return 0

    lax.fori_loop(0, count, one, 0)
    if not first:
        scaled = scalars[0] * part[...]
        part[...] = scaled
        sent[...] = scaled.astype(BF16)


def pair_tiles(scalars, images, texts, before, tokens, batch_total):
    first = before is None
    count, width = images.shape
    block = 256
    outs = [jax.ShapeDtypeStruct((count, width), F32)]
    if not first:
        outs.append(jax.ShapeDtypeStruct((count, width), BF16))
    outs.append(jax.ShapeDtypeStruct((1, block), F32))
    pairs = count * texts.shape[0]
    return pl.pallas_call(
        functools.partial(
            pair_kernel, first=first, tokens=tokens, batch_total=batch_total, block=block
        ),
        in_specs=[pl.BlockSpec(memory_space=pltpu.SMEM)]
        + [pl.BlockSpec(memory_space=pltpu.VMEM)] * (2 if first else 3),
        out_shape=outs,
        scratch_shapes=[pltpu.VMEM((2, count, block), F32)],
        cost_estimate=pl.CostEstimate(
            flops=4 * pairs * width, bytes_accessed=2 * texts.size, transcendentals=3 * pairs
        ),
    )(scalars, images, texts, *([] if first else [before]))


def step(pooled, hidden, text, weight, row_moment, col_moment, log_scale, bias):
    tokens = pooled.shape[0]
    batch_total = tokens * 256
    slice_ff = weight.shape[1]
    k_place = lax.axis_index("k")

    quarter = D // 4
    x_place = lax.axis_index("x")
    y_place = lax.axis_index("y")
    half_ff = slice_ff

    text_float = text.astype(F32)
    text_units = (
        text_float / jnp.sqrt(jnp.sum(text_float * text_float, axis=1, keepdims=True) + EPSILON)
    ).astype(BF16)
    texts_y = joined([text_units] + [shift(text_units, k=1, y=s) for s in (1, 2, 3)])

    by_slice = jnp.moveaxis(hidden.reshape(tokens, 8, half_ff), 1, 0).reshape(
        4, 2, tokens, half_ff
    )
    by_slice = jnp.where(k_place == 0, by_slice, by_slice[:, ::-1])
    hid_mine = rolled(by_slice, x_place, 4)
    hid_y = [hid_mine] + [shift(hid_mine, y=-s) for s in (1, 2, 3)]

    up, down = ring_step(texts_y, texts_y, "z")
    ring_pieces = [texts_y, up, down]

    weight_z = everywhere(weight.astype(BF16), "z").reshape(quarter, half_ff)
    weight_own = [weight_z] + [shift(weight_z, x=-s) for s in (1, 2, 3)]
    weight_own = joined([w[None] for w in weight_own])
    weight_other = shift(after(weight_own, up, down), k=1)
    up, down = ring_step(up, down, "z")
    ring_pieces += [up, down]
    mixed_part, *hid_all = project(hid_y, weight_own, weight_other)
    mixed_part = mixed_part.reshape(4, tokens, quarter)

    by_y = (2, 4, tokens, half_ff)
    hid_x = [hid_all[0]] + [
        shift(hid_all[s].reshape(by_y), x=s, k=1).reshape(hid_all[s].shape)
        for s in (1, 2, 3)
    ]
    arrived = exchange(rolled(mixed_part, -y_place, 4), "y")
    mixed = pooled.astype(F32) + jnp.moveaxis(arrived, 0, 1).reshape(tokens, D)
    length = jnp.sqrt(jnp.sum(mixed * mixed, axis=1, keepdims=True) + EPSILON)
    unit = mixed / length
    images = unit.astype(BF16)
    up, down = ring_step(*after((up, down), mixed_part), "z")
    ring_pieces += [up, down]
    half = texts_y.shape[0] // 2
    ring_pieces += ring_step(*after((up[:half], down[half:]), images), "z")

    logit_scale = jnp.exp(log_scale)
    image_rows = joined([images] + [shift(images, x=s) for s in (1, 2, 3)])
    texts_own = jnp.concatenate(ring_pieces[:-2] + after(ring_pieces[-2:], image_rows))
    texts_other = shift(texts_own, k=1)
    scalars = jnp.stack([logit_scale, bias])
    part_a, loss_a = pair_tiles(scalars, image_rows, texts_own, None, tokens, batch_total)
    part, part_sent, loss_b = pair_tiles(
        scalars, image_rows, texts_other, part_a, tokens, batch_total
    )
    unit_grad = part[:tokens] + sum(
        shift(part_sent[s * tokens : (s + 1) * tokens], x=-s).astype(F32) for s in (1, 2, 3)
    )
    mixed_grad = (
        (unit_grad - unit * jnp.sum(unit * unit_grad, axis=1, keepdims=True)) / length
    ).astype(BF16)

    quarters = jnp.moveaxis(mixed_grad.reshape(tokens, 4, quarter), 1, 0)
    quarters = rolled(quarters, y_place, 4)
    grad_y = [quarters[0]] + [shift(quarters[s], y=s) for s in (1, 2, 3)]
    grad_mine = joined([grad_y[-s] for s in range(4)])
    grad_x = [grad_mine] + [shift(grad_mine, x=s, k=1) for s in (1, 2, 3)]
    both = gradients(grad_x, hid_x)
    chip_grad = both[0] + shift(both[1], k=1)
    arrived_grad = exchange(chip_grad.astype(BF16).reshape(8, D // 32, slice_ff), "z")
    gradient = jnp.sum(arrived_grad.astype(F32), axis=0)

    squared = gradient * gradient + FLOOR_VALUE
    row_message = jnp.concatenate([jnp.sum(squared, axis=1), jnp.sum(loss_a + loss_b).reshape(1)])
    row_total = jnp.sum(everywhere(row_message[None], ROW), axis=(0, 1))
    loss_row = row_total[-1]
    new_row = DECAY_RATE * row_moment + (1.0 - DECAY_RATE) * row_total[:-1] / FF
    scaled = jnp.sum(gradient * gradient / new_row[:, None], axis=0)
    col_message = jnp.stack(
        [jnp.sum(squared, axis=0), scaled, jnp.full((slice_ff,), loss_row)]
    )
    col_total = jnp.sum(everywhere(col_message, COL), axis=0)
    new_col = DECAY_RATE * col_moment + (1.0 - DECAY_RATE) * col_total[0] / D
    loss = col_total[2, 0] / batch_total
    ours = jnp.sum(col_total[1] / new_col)
    update_total = jnp.sum(everywhere(jnp.full((1, 128), ours), ROW), axis=(0, 1))[0]
    update_rms = jnp.sqrt(update_total / (D * FF))
    raw_update = gradient / jnp.sqrt(new_row[:, None] * new_col[None, :])
    update = raw_update / jnp.maximum(1.0, update_rms / CLIP_LEVEL)
    return (update, new_row, new_col, loss)


def solution(mesh):
    finer = Mesh(mesh.devices.reshape(4, 2, 4, 8), AXES)
    return jax.shard_map(
        step,
        mesh=finer,
        in_specs=(
            P(AXES, None),
            P(AXES, None),
            P(AXES, None),
            P(COL, ROW),
            P(COL),
            P(ROW),
            P(),
            P(),
        ),
        out_specs=(P(COL, ROW), P(COL), P(ROW), P()),
        check_vma=False,
    )
```

```python
import functools
import itertools

import jax
import jax.numpy as jnp
from jax import lax
from jax.experimental import pallas as pl
from jax.experimental.pallas import tpu as pltpu
from jax.sharding import Mesh
from jax.sharding import PartitionSpec as P


D = 1152
FF = 4304
AXES = ("x", "k", "y", "z")
SIZES = {"x": 4, "k": 2, "y": 4, "z": 8}
ROW = ("x", "k")
COL = ("y", "z")
EPSILON = 1e-06
DECAY_RATE = 0.8
CLIP_LEVEL = 1.0
FLOOR_VALUE = 1e-30
BF16 = jnp.bfloat16
F32 = jnp.float32


def shift(value, **by):
    names = tuple(a for a in AXES if a in by)
    sizes = [SIZES[a] for a in names]

    def linear(place):
        index = 0
        for p, n in zip(place, sizes):
            index = index * n + p
        return index

    pairs = [
        (linear(p), linear([(c + by[a]) % SIZES[a] for c, a in zip(p, names)]))
        for p in itertools.product(*[range(n) for n in sizes])
    ]
    return lax.ppermute(value, names, pairs)


def exchange(pieces, axes):
    return lax.all_to_all(pieces, axes, split_axis=0, concat_axis=0, tiled=True)


def everywhere(array, axes):
    return exchange(jnp.broadcast_to(array, (lax.axis_size(axes), *array.shape)), axes)


def rolled(pieces, by, count):
    twice = jnp.concatenate([pieces, pieces])
    return lax.dynamic_slice_in_dim(twice, by & (count - 1), count, 0)


def ring_step(up, down, axis):
    return shift(up, **{axis: 1}), shift(down, **{axis: -1})


def project_kernel(h0, h1, h2, h3, own, other, part, *hid):
    at = pl.program_id(0)
    total = None
    for kk in range(2):
        rows = jnp.concatenate([h[0, kk] for h in (h0, h1, h2, h3)], axis=0)
        for s in range(4):

            @pl.when(at == s)
            def _(s=s, rows=rows):
                hid[s][kk] = rows

        piece = lax.dot_general(
            rows, (own, other)[kk][0], (((1,), (1,)), ((), ())), preferred_element_type=F32
        )
        total = piece if total is None else total + piece

    @pl.when(at == 0)
    def _():
        part[...] = total

    @pl.when(at > 0)
    def _():
        part[...] += total


def project(hid_y, own, other):
    count, _, tokens, units = hid_y[0].shape
    features = own.shape[1]
    weights = pl.BlockSpec((1, features, units), lambda i: (i, 0, 0))
    rows = (2, 4 * tokens, units)
    return pl.pallas_call(
        project_kernel,
        grid=(count,),
        in_specs=[pl.BlockSpec((1, 2, tokens, units), lambda i: (i, 0, 0, 0))] * 4
        + [weights] * 2,
        out_specs=[pl.BlockSpec((4 * tokens, features), lambda i: (0, 0))]
        + [pl.BlockSpec(rows, lambda i: (0, 0, 0))] * 4,
        out_shape=[jax.ShapeDtypeStruct((4 * tokens, features), F32)]
        + [jax.ShapeDtypeStruct(rows, BF16)] * 4,
        cost_estimate=pl.CostEstimate(
            flops=2 * count * 2 * 4 * tokens * units * features,
            bytes_accessed=8000000,
            transcendentals=0,
        ),
        compiler_params=pltpu.CompilerParams(dimension_semantics=("arbitrary",)),
    )(*hid_y, own, other)


def gradient_kernel(*refs):
    grads, hid, outs = refs[:4], refs[4:8], refs[8:]
    total = None
    for s in range(4):
        piece = jnp.dot(grads[s][...].T, hid[s][0], preferred_element_type=F32)
        total = piece if total is None else total + piece
    for kk in range(2):

        @pl.when(pl.program_id(0) == kk)
        def _(kk=kk):
            outs[kk][...] = total


def gradients(grads, hid):
    tokens, features = grads[0].shape
    units = hid[0].shape[2]
    whole = pl.BlockSpec((features, units), lambda i: (0, 0))
    return pl.pallas_call(
        gradient_kernel,
        grid=(2,),
        in_specs=[pl.BlockSpec((tokens, features), lambda i: (0, 0))] * 4
        + [pl.BlockSpec((1, tokens, units), lambda i: (i, 0, 0))]
        + [pl.BlockSpec((1, tokens, units), lambda i: (1 - i, 0, 0))] * 3,
        out_specs=[whole] * 2,
        out_shape=[jax.ShapeDtypeStruct((features, units), F32)] * 2,
        cost_estimate=pl.CostEstimate(
            flops=16 * grads[0].size * units, bytes_accessed=4000000, transcendentals=0
        ),
        compiler_params=pltpu.CompilerParams(dimension_semantics=("arbitrary",)),
    )(*grads, *hid)


def joined(pieces):
    rows = sum(p.shape[0] for p in pieces)
    whole = jnp.zeros((rows, *pieces[0].shape[1:]), pieces[0].dtype)
    at = 0
    for piece in pieces:
        whole = lax.dynamic_update_slice_in_dim(whole, piece, at, 0)
        at += piece.shape[0]
    return whole


def pair_kernel(scalars, images, texts, *refs, first, tokens, batch_total, block):
    if first:
        part, loss, kept = refs
        part[...] = jnp.zeros(part.shape, F32)
    else:
        before, part, sent, loss, kept = refs
        part[...] = before[...]
    loss[...] = jnp.zeros(loss.shape, F32)
    count = texts.shape[0] // block

    def block_of(at):
        return texts[pl.ds(pl.multiple_of(at * block, block), block), :]

    def logits_of(at):
        return (
            scalars[0]
            * lax.dot_general(
                images[...], block_of(at), (((1,), (1,)), ((), ())), preferred_element_type=F32
            )
            + scalars[1]
        )

    kept[0] = logits_of(0)

    def one(at, _):
        logits = kept[at & 1]
        kept[(at + 1) & 1] = logits_of(jnp.minimum(at + 1, count - 1))
        if first:
            rows = lax.broadcasted_iota(jnp.int32, logits.shape, 0)
            cols = lax.broadcasted_iota(jnp.int32, logits.shape, 1) + at * block
            positive = (rows == cols) & (rows < tokens)
            logits = jnp.where(positive, -logits, logits)
        small = jnp.exp(-jnp.abs(logits))
        base = 1.0 + small
        inverse = 1.0 / base
        slope = jnp.where(logits >= 0, inverse, small * inverse) / batch_total
        if first:
            slope = jnp.where(positive, -slope, slope)
        part[...] += jnp.dot(
            slope.astype(BF16), block_of(at), preferred_element_type=F32
        )
        softplus = jnp.maximum(logits, 0.0) + (
            jnp.log(base) + (small - (base - 1.0)) * inverse
        )
        loss[...] += jnp.sum(softplus, axis=0, keepdims=True)
        return 0

    lax.fori_loop(0, count, one, 0)
    if not first:
        scaled = scalars[0] * part[...]
        part[...] = scaled
        sent[...] = scaled.astype(BF16)


def pair_tiles(scalars, images, texts, before, tokens, batch_total):
    first = before is None
    count, width = images.shape
    block = 256
    outs = [jax.ShapeDtypeStruct((count, width), F32)]
    if not first:
        outs.append(jax.ShapeDtypeStruct((count, width), BF16))
    outs.append(jax.ShapeDtypeStruct((1, block), F32))
    pairs = count * texts.shape[0]
    return pl.pallas_call(
        functools.partial(
            pair_kernel, first=first, tokens=tokens, batch_total=batch_total, block=block
        ),
        in_specs=[pl.BlockSpec(memory_space=pltpu.SMEM)]
        + [pl.BlockSpec(memory_space=pltpu.VMEM)] * (2 if first else 3),
        out_shape=outs,
        scratch_shapes=[pltpu.VMEM((2, count, block), F32)],
        cost_estimate=pl.CostEstimate(
            flops=4 * pairs * width, bytes_accessed=2 * texts.size, transcendentals=3 * pairs
        ),
    )(scalars, images, texts, *([] if first else [before]))


def step(pooled, hidden, text, weight, row_moment, col_moment, log_scale, bias):
    tokens = pooled.shape[0]
    batch_total = tokens * 256
    slice_ff = weight.shape[1]
    k_place = lax.axis_index("k")

    quarter = D // 4
    x_place = lax.axis_index("x")
    y_place = lax.axis_index("y")
    half_ff = slice_ff

    text_float = text.astype(F32)
    text_units = (
        text_float / jnp.sqrt(jnp.sum(text_float * text_float, axis=1, keepdims=True) + EPSILON)
    ).astype(BF16)
    texts_y = joined([text_units] + [shift(text_units, k=1, y=s) for s in (1, 2, 3)])

    by_slice = jnp.moveaxis(hidden.reshape(tokens, 8, half_ff), 1, 0).reshape(
        4, 2, tokens, half_ff
    )
    by_slice = jnp.where(k_place == 0, by_slice, by_slice[:, ::-1])
    hid_mine = rolled(by_slice, x_place, 4)
    hid_y = [hid_mine] + [shift(hid_mine, y=-s) for s in (1, 2, 3)]

    up, down = ring_step(texts_y, texts_y, "z")
    ring_pieces = [texts_y, up, down]
    up, down = ring_step(up, down, "z")
    ring_pieces += [up, down]
    up, down = ring_step(up, down, "z")
    ring_pieces += [up, down]
    half = texts_y.shape[0] // 2
    ring_pieces += ring_step(up[:half], down[half:], "z")

    weight_z = everywhere(weight.astype(BF16), "z").reshape(quarter, half_ff)
    weight_own = [weight_z] + [shift(weight_z, x=-s) for s in (1, 2, 3)]
    weight_own = joined([w[None] for w in weight_own])
    weight_other = shift(weight_own, k=1)
    mixed_part, *hid_all = project(hid_y, weight_own, weight_other)
    mixed_part = mixed_part.reshape(4, tokens, quarter)

    by_y = (2, 4, tokens, half_ff)
    hid_x = [hid_all[0]] + [
        shift(hid_all[s].reshape(by_y), x=s, k=1).reshape(hid_all[s].shape)
        for s in (1, 2, 3)
    ]
    arrived = exchange(rolled(mixed_part, -y_place, 4), "y")
    mixed = pooled.astype(F32) + jnp.moveaxis(arrived, 0, 1).reshape(tokens, D)
    length = jnp.sqrt(jnp.sum(mixed * mixed, axis=1, keepdims=True) + EPSILON)
    unit = mixed / length
    images = unit.astype(BF16)

    logit_scale = jnp.exp(log_scale)
    image_rows = joined([images] + [shift(images, x=s) for s in (1, 2, 3)])
    texts_own = jnp.concatenate(ring_pieces)
    texts_other = shift(texts_own, k=1)
    scalars = jnp.stack([logit_scale, bias])
    part_a, loss_a = pair_tiles(scalars, image_rows, texts_own, None, tokens, batch_total)
    part, part_sent, loss_b = pair_tiles(
        scalars, image_rows, texts_other, part_a, tokens, batch_total
    )
    unit_grad = part[:tokens] + sum(
        shift(part_sent[s * tokens : (s + 1) * tokens], x=-s).astype(F32) for s in (1, 2, 3)
    )
    mixed_grad = (
        (unit_grad - unit * jnp.sum(unit * unit_grad, axis=1, keepdims=True)) / length
    ).astype(BF16)

    quarters = jnp.moveaxis(mixed_grad.reshape(tokens, 4, quarter), 1, 0)
    quarters = rolled(quarters, y_place, 4)
    grad_y = [quarters[0]] + [shift(quarters[s], y=s) for s in (1, 2, 3)]
    grad_mine = joined([grad_y[-s] for s in range(4)])
    grad_x = [grad_mine] + [shift(grad_mine, x=s, k=1) for s in (1, 2, 3)]
    both = gradients(grad_x, hid_x)
    chip_grad = both[0] + shift(both[1], k=1)
    arrived_grad = exchange(chip_grad.astype(BF16).reshape(8, D // 32, slice_ff), "z")
    gradient = jnp.sum(arrived_grad.astype(F32), axis=0)

    squared = gradient * gradient + FLOOR_VALUE
    row_message = jnp.concatenate([jnp.sum(squared, axis=1), jnp.sum(loss_a + loss_b).reshape(1)])
    row_total = jnp.sum(everywhere(row_message[None], ROW), axis=(0, 1))
    loss_row = row_total[-1]
    new_row = DECAY_RATE * row_moment + (1.0 - DECAY_RATE) * row_total[:-1] / FF
    scaled = jnp.sum(gradient * gradient / new_row[:, None], axis=0)
    col_message = jnp.concatenate(
        [jnp.sum(squared, axis=0), scaled, loss_row.reshape(1)]
    ).reshape(1, 2 * slice_ff + 1)
    col_total = jnp.sum(everywhere(col_message, COL), axis=(0, 1))
    new_col = DECAY_RATE * col_moment + (1.0 - DECAY_RATE) * col_total[:slice_ff] / D
    loss = col_total[-1] / batch_total
    ours = jnp.sum(col_total[slice_ff:-1] / new_col)
    update_total = jnp.sum(everywhere(jnp.full((1, 128), ours), ROW), axis=(0, 1))[0]
    update_rms = jnp.sqrt(update_total / (D * FF))
    raw_update = gradient / jnp.sqrt(new_row[:, None] * new_col[None, :])
    update = raw_update / jnp.maximum(1.0, update_rms / CLIP_LEVEL)
    return (update, new_row, new_col, loss)


def solution(mesh):
    finer = Mesh(mesh.devices.reshape(4, 2, 4, 8), AXES)
    return jax.shard_map(
        step,
        mesh=finer,
        in_specs=(
            P(AXES, None),
            P(AXES, None),
            P(AXES, None),
            P(COL, ROW),
            P(COL),
            P(ROW),
            P(),
            P(),
        ),
        out_specs=(P(COL, ROW), P(COL), P(ROW), P()),
        check_vma=False,
    )
```

```python
import functools
import itertools

import jax
import jax.numpy as jnp
from jax import lax
from jax.experimental import pallas as pl
from jax.experimental.pallas import tpu as pltpu
from jax.sharding import Mesh
from jax.sharding import PartitionSpec as P


D = 1152
FF = 4304
AXES = ("x", "k", "y", "z")
SIZES = {"x": 4, "k": 2, "y": 4, "z": 8}
ROW = ("x", "k")
COL = ("y", "z")
EPSILON = 1e-06
DECAY_RATE = 0.8
CLIP_LEVEL = 1.0
FLOOR_VALUE = 1e-30
BF16 = jnp.bfloat16
F32 = jnp.float32


def shift(value, **by):
    names = tuple(a for a in AXES if a in by)
    sizes = [SIZES[a] for a in names]

    def linear(place):
        index = 0
        for p, n in zip(place, sizes):
            index = index * n + p
        return index

    pairs = [
        (linear(p), linear([(c + by[a]) % SIZES[a] for c, a in zip(p, names)]))
        for p in itertools.product(*[range(n) for n in sizes])
    ]
    return lax.ppermute(value, names, pairs)


def exchange(pieces, axes):
    return lax.all_to_all(pieces, axes, split_axis=0, concat_axis=0, tiled=True)


def everywhere(array, axes):
    return exchange(jnp.broadcast_to(array, (lax.axis_size(axes), *array.shape)), axes)


def after(values, *others):
    return lax.optimization_barrier((values, others))[0]


def ring_step(up, down, axis):
    return shift(up, **{axis: 1}), shift(down, **{axis: -1})


def joined(pieces):
    rows = sum(p.shape[0] for p in pieces)
    whole = jnp.zeros((rows, *pieces[0].shape[1:]), pieces[0].dtype)
    at = 0
    for piece in pieces:
        whole = lax.dynamic_update_slice_in_dim(whole, piece, at, 0)
        at += piece.shape[0]
    return whole


def pair_kernel(scalars, images, texts, *refs, first, tokens, batch_total, block):
    if first:
        part, loss, kept = refs
        part[...] = jnp.zeros(part.shape, F32)
    else:
        before, part, sent, loss, kept = refs
        part[...] = before[...]
    loss[...] = jnp.zeros(loss.shape, F32)
    count = texts.shape[0] // block

    def block_of(at):
        return texts[pl.ds(pl.multiple_of(at * block, block), block), :]

    def logits_of(at):
        return (
            scalars[0]
            * lax.dot_general(
                images[...], block_of(at), (((1,), (1,)), ((), ())), preferred_element_type=F32
            )
            + scalars[1]
        )

    kept[0] = logits_of(0)

    def one(at, _):
        logits = kept[at & 1]
        kept[(at + 1) & 1] = logits_of(jnp.minimum(at + 1, count - 1))
        if first:
            rows = lax.broadcasted_iota(jnp.int32, logits.shape, 0)
            cols = lax.broadcasted_iota(jnp.int32, logits.shape, 1) + at * block
            positive = (rows == cols) & (rows < tokens)
            logits = jnp.where(positive, -logits, logits)
        small = jnp.exp(-jnp.abs(logits))
        base = 1.0 + small
        inverse = 1.0 / base
        slope = jnp.where(logits >= 0, inverse, small * inverse) / batch_total
        if first:
            slope = jnp.where(positive, -slope, slope)
        part[...] += jnp.dot(
            slope.astype(BF16), block_of(at), preferred_element_type=F32
        )
        softplus = jnp.maximum(logits, 0.0) + (
            jnp.log(base) + (small - (base - 1.0)) * inverse
        )
        loss[...] += jnp.sum(softplus, axis=0, keepdims=True)
        return 0

    lax.fori_loop(0, count, one, 0)
    if not first:
        scaled = scalars[0] * part[...]
        part[...] = scaled
        sent[...] = scaled.astype(BF16)


def pair_tiles(scalars, images, texts, before, tokens, batch_total):
    first = before is None
    count, width = images.shape
    block = 512
    outs = [jax.ShapeDtypeStruct((count, width), F32)]
    if not first:
        outs.append(jax.ShapeDtypeStruct((count, width), BF16))
    outs.append(jax.ShapeDtypeStruct((1, block), F32))
    pairs = count * texts.shape[0]
    return pl.pallas_call(
        functools.partial(
            pair_kernel, first=first, tokens=tokens, batch_total=batch_total, block=block
        ),
        in_specs=[pl.BlockSpec(memory_space=pltpu.SMEM)]
        + [pl.BlockSpec(memory_space=pltpu.VMEM)] * (2 if first else 3),
        out_shape=outs,
        scratch_shapes=[pltpu.VMEM((2, count, block), F32)],
        cost_estimate=pl.CostEstimate(
            flops=4 * pairs * width, bytes_accessed=2 * texts.size, transcendentals=3 * pairs
        ),
    )(scalars, images, texts, *([] if first else [before]))


def step(pooled, hidden, text, weight, row_moment, col_moment, log_scale, bias):
    tokens = pooled.shape[0]
    batch_total = tokens * 256
    slice_ff = weight.shape[1]
    k_place = lax.axis_index("k")

    first_core = k_place == 0
    quarter = D // 4
    x_place = lax.axis_index("x")
    hidden_by_x = jnp.moveaxis(hidden.reshape(tokens, 4, 2 * slice_ff), 1, 0)
    hidden_x = jnp.zeros((4, tokens, 2 * slice_ff), BF16)
    for s in range(4):
        piece = lax.dynamic_index_in_dim(hidden_by_x, (x_place + s) & 3, 0, keepdims=True)
        if s > 0:
            piece = shift(piece, x=s)
        hidden_x = lax.dynamic_update_index_in_dim(hidden_x, piece, (x_place - s) & 3, 0)
    hidden_x = hidden_x.reshape(4 * tokens, 2 * slice_ff)
    hid_y = [hidden_x] + [shift(hidden_x, y=-s) for s in (1, 2, 3)]

    text_float = text.astype(F32)
    text_units = (
        text_float / jnp.sqrt(jnp.sum(text_float * text_float, axis=1, keepdims=True) + EPSILON)
    ).astype(BF16)
    texts_y = joined([text_units] + [shift(text_units, k=1, y=s) for s in (1, 2, 3)])
    up, down = ring_step(texts_y, texts_y, "z")
    ring_pieces = [texts_y, up, down]
    up, down = ring_step(up, down, "z")
    ring_pieces += [up, down]

    weight_own = everywhere(weight.astype(BF16), "z").reshape(quarter, slice_ff)
    weight_other = shift(weight_own, k=1)
    weight_x = jnp.concatenate(
        [
            jnp.where(first_core, weight_own, weight_other),
            jnp.where(first_core, weight_other, weight_own),
        ],
        axis=1,
    )
    partial = jnp.stack(
        [
            lax.dot_general(
                piece, weight_x, (((1,), (1,)), ((), ())), preferred_element_type=F32
            )
            .astype(BF16)
            .reshape(4, tokens, quarter)
            for piece in hid_y
        ]
    )
    y_place = lax.axis_index("y")
    partial = jnp.stack(
        [
            lax.dynamic_index_in_dim(partial, (c - y_place) & 3, 0, keepdims=False)
            for c in range(4)
        ],
        axis=1,
    )
    up, down = ring_step(*after((up, down), partial), "z")
    ring_pieces += [up, down]
    arrived = exchange(partial.reshape(16, tokens, quarter), ("x", "y"))
    half = texts_y.shape[0] // 2
    up, down = after((up, down), arrived)
    ring_pieces += ring_step(up[:half], down[half:], "z")
    projected = jnp.sum(arrived.astype(F32).reshape(4, 4, tokens, quarter), axis=0)
    mixed = pooled.astype(F32) + jnp.moveaxis(projected, 0, 1).reshape(tokens, D)
    length = jnp.sqrt(jnp.sum(mixed * mixed, axis=1, keepdims=True) + EPSILON)
    unit = mixed / length
    images = unit.astype(BF16)
    logit_scale = jnp.exp(log_scale)
    image_rows = joined([images] + [shift(images, x=s) for s in (1, 2, 3)])
    texts_own = jnp.concatenate(ring_pieces[:-2] + after(ring_pieces[-2:], image_rows))
    texts_other = shift(texts_own, k=1)
    scalars = jnp.stack([logit_scale, bias])
    part_a, loss_a = pair_tiles(scalars, image_rows, texts_own, None, tokens, batch_total)
    part, part_sent, loss_b = pair_tiles(
        scalars, image_rows, texts_other, part_a, tokens, batch_total
    )
    unit_grad = part[:tokens] + sum(
        shift(part_sent[s * tokens : (s + 1) * tokens], x=-s).astype(F32) for s in (1, 2, 3)
    )
    mixed_grad = (
        (unit_grad - unit * jnp.sum(unit * unit_grad, axis=1, keepdims=True)) / length
    ).astype(BF16)

    quarters = jnp.moveaxis(mixed_grad.reshape(tokens, 4, quarter), 1, 0)
    grad_rows = exchange(
        jnp.broadcast_to(quarters[None], (4, 4, tokens, quarter)).reshape(16, tokens, quarter),
        ("x", "y"),
    ).reshape(4, 4, tokens, quarter)
    grad_by_y = jnp.moveaxis(grad_rows, 1, 0).reshape(4, 4 * tokens, quarter)
    both = F32(0.0)
    for s in range(4):
        part = lax.dynamic_index_in_dim(grad_by_y, (y_place + s) & 3, 0, keepdims=False)
        both = both + lax.dot_general(
            part, hid_y[s], (((0,), (0,)), ((), ())), preferred_element_type=F32
        )
    low, high = both[:, :slice_ff], both[:, slice_ff:]
    chip_grad = jnp.where(first_core, low, high) + shift(jnp.where(first_core, high, low), k=1)
    arrived_grad = exchange(chip_grad.astype(BF16).reshape(8, D // 32, slice_ff), "z")
    gradient = jnp.sum(arrived_grad.astype(F32), axis=0)

    squared = gradient * gradient + FLOOR_VALUE
    row_message = jnp.concatenate([jnp.sum(squared, axis=1), jnp.sum(loss_a + loss_b).reshape(1)])
    row_total = jnp.sum(everywhere(row_message[None], ROW), axis=(0, 1))
    loss_row = row_total[-1]
    new_row = DECAY_RATE * row_moment + (1.0 - DECAY_RATE) * row_total[:-1] / FF
    scaled = jnp.sum(gradient * gradient / new_row[:, None], axis=0)
    col_message = jnp.concatenate(
        [jnp.sum(squared, axis=0), scaled, loss_row.reshape(1)]
    ).reshape(1, 2 * slice_ff + 1)
    col_total = jnp.sum(everywhere(col_message, COL), axis=(0, 1))
    new_col = DECAY_RATE * col_moment + (1.0 - DECAY_RATE) * col_total[:slice_ff] / D
    loss = col_total[-1] / batch_total
    ours = jnp.sum(col_total[slice_ff:-1] / new_col)
    update_total = jnp.sum(everywhere(jnp.full((1, 128), ours), ROW), axis=(0, 1))[0]
    update_rms = jnp.sqrt(update_total / (D * FF))
    raw_update = gradient / jnp.sqrt(new_row[:, None] * new_col[None, :])
    update = raw_update / jnp.maximum(1.0, update_rms / CLIP_LEVEL)
    return (update, new_row, new_col, loss)


def solution(mesh):
    finer = Mesh(mesh.devices.reshape(4, 2, 4, 8), AXES)
    return jax.shard_map(
        step,
        mesh=finer,
        in_specs=(
            P(AXES, None),
            P(AXES, None),
            P(AXES, None),
            P(COL, ROW),
            P(COL),
            P(ROW),
            P(),
            P(),
        ),
        out_specs=(P(COL, ROW), P(COL), P(ROW), P()),
        check_vma=False,
    )
```

```python
import functools
import itertools

import jax
import jax.numpy as jnp
from jax import lax
from jax.experimental import pallas as pl
from jax.experimental.pallas import tpu as pltpu
from jax.sharding import Mesh
from jax.sharding import PartitionSpec as P


D = 1152
FF = 4304
AXES = ("x", "k", "y", "z")
SIZES = {"x": 4, "k": 2, "y": 4, "z": 8}
ROW = ("x", "k")
COL = ("y", "z")
EPSILON = 1e-06
DECAY_RATE = 0.8
CLIP_LEVEL = 1.0
FLOOR_VALUE = 1e-30
BF16 = jnp.bfloat16
F32 = jnp.float32


def shift(value, **by):
    names = tuple(a for a in AXES if a in by)
    sizes = [SIZES[a] for a in names]

    def linear(place):
        index = 0
        for p, n in zip(place, sizes):
            index = index * n + p
        return index

    pairs = [
        (linear(p), linear([(c + by[a]) % SIZES[a] for c, a in zip(p, names)]))
        for p in itertools.product(*[range(n) for n in sizes])
    ]
    return lax.ppermute(value, names, pairs)


def exchange(pieces, axes):
    return lax.all_to_all(pieces, axes, split_axis=0, concat_axis=0, tiled=True)


def everywhere(array, axes):
    return exchange(jnp.broadcast_to(array, (lax.axis_size(axes), *array.shape)), axes)


def after(values, *others):
    return lax.optimization_barrier((values, others))[0]


def ring_step(up, down, axis):
    return shift(up, **{axis: 1}), shift(down, **{axis: -1})


def joined(pieces):
    rows = sum(p.shape[0] for p in pieces)
    whole = jnp.zeros((rows, *pieces[0].shape[1:]), pieces[0].dtype)
    at = 0
    for piece in pieces:
        whole = lax.dynamic_update_slice_in_dim(whole, piece, at, 0)
        at += piece.shape[0]
    return whole


def pair_kernel(scalars, images, texts, *refs, first, tokens, batch_total, block):
    if first:
        part, loss, kept = refs
        part[...] = jnp.zeros(part.shape, F32)
    else:
        before, part, sent, loss, kept = refs
        part[...] = before[...]
    loss[...] = jnp.zeros(loss.shape, F32)
    count = texts.shape[0] // block

    def block_of(at):
        return texts[pl.ds(pl.multiple_of(at * block, block), block), :]

    def logits_of(at):
        return (
            scalars[0]
            * lax.dot_general(
                images[...], block_of(at), (((1,), (1,)), ((), ())), preferred_element_type=F32
            )
            + scalars[1]
        )

    kept[0] = logits_of(0)

    def one(at, _):
        logits = kept[at & 1]
        kept[(at + 1) & 1] = logits_of(jnp.minimum(at + 1, count - 1))
        if first:
            rows = lax.broadcasted_iota(jnp.int32, logits.shape, 0)
            cols = lax.broadcasted_iota(jnp.int32, logits.shape, 1) + at * block
            positive = (rows == cols) & (rows < tokens)
            logits = jnp.where(positive, -logits, logits)
        small = jnp.exp(-jnp.abs(logits))
        base = 1.0 + small
        inverse = 1.0 / base
        slope = jnp.where(logits >= 0, inverse, small * inverse) / batch_total
        if first:
            slope = jnp.where(positive, -slope, slope)
        part[...] += jnp.dot(
            slope.astype(BF16), block_of(at), preferred_element_type=F32
        )
        softplus = jnp.maximum(logits, 0.0) + (
            jnp.log(base) + (small - (base - 1.0)) * inverse
        )
        loss[...] += jnp.sum(softplus, axis=0, keepdims=True)
        return 0

    lax.fori_loop(0, count, one, 0, unroll=2)
    if not first:
        scaled = scalars[0] * part[...]
        part[...] = scaled
        sent[...] = scaled.astype(BF16)


def pair_tiles(scalars, images, texts, before, tokens, batch_total):
    first = before is None
    count, width = images.shape
    block = 512
    outs = [jax.ShapeDtypeStruct((count, width), F32)]
    if not first:
        outs.append(jax.ShapeDtypeStruct((count, width), BF16))
    outs.append(jax.ShapeDtypeStruct((1, block), F32))
    pairs = count * texts.shape[0]
    return pl.pallas_call(
        functools.partial(
            pair_kernel, first=first, tokens=tokens, batch_total=batch_total, block=block
        ),
        in_specs=[pl.BlockSpec(memory_space=pltpu.SMEM)]
        + [pl.BlockSpec(memory_space=pltpu.VMEM)] * (2 if first else 3),
        out_shape=outs,
        scratch_shapes=[pltpu.VMEM((2, count, block), F32)],
        cost_estimate=pl.CostEstimate(
            flops=4 * pairs * width, bytes_accessed=2 * texts.size, transcendentals=3 * pairs
        ),
    )(scalars, images, texts, *([] if first else [before]))


def step(pooled, hidden, text, weight, row_moment, col_moment, log_scale, bias):
    tokens = pooled.shape[0]
    batch_total = tokens * 256
    slice_ff = weight.shape[1]
    k_place = lax.axis_index("k")

    first_core = k_place == 0
    quarter = D // 4
    x_place = lax.axis_index("x")
    hidden_by_x = jnp.moveaxis(hidden.reshape(tokens, 4, 2 * slice_ff), 1, 0)
    hidden_x = jnp.zeros((4, tokens, 2 * slice_ff), BF16)
    for s in range(4):
        piece = lax.dynamic_index_in_dim(hidden_by_x, (x_place + s) & 3, 0, keepdims=True)
        if s > 0:
            piece = shift(piece, x=s)
        hidden_x = lax.dynamic_update_index_in_dim(hidden_x, piece, (x_place - s) & 3, 0)
    hidden_x = hidden_x.reshape(4 * tokens, 2 * slice_ff)
    hid_y = [hidden_x] + [shift(hidden_x, y=-s) for s in (1, 2, 3)]

    text_float = text.astype(F32)
    text_units = (
        text_float / jnp.sqrt(jnp.sum(text_float * text_float, axis=1, keepdims=True) + EPSILON)
    ).astype(BF16)
    texts_y = joined([text_units] + [shift(text_units, k=1, y=s) for s in (1, 2, 3)])
    up, down = ring_step(texts_y, texts_y, "z")
    ring_pieces = [texts_y, up, down]
    up, down = ring_step(up, down, "z")
    ring_pieces += [up, down]

    scalars = jnp.stack([jnp.exp(log_scale), bias])
    weight_own = everywhere(after(weight.astype(BF16), hidden_x), "z")
    weight_own = after(weight_own.reshape(quarter, slice_ff), scalars)
    weight_other = shift(weight_own, k=1)
    weight_x = jnp.concatenate(
        [
            jnp.where(first_core, weight_own, weight_other),
            jnp.where(first_core, weight_other, weight_own),
        ],
        axis=1,
    )
    partial = jnp.stack(
        [
            lax.dot_general(
                piece, weight_x, (((1,), (1,)), ((), ())), preferred_element_type=F32
            )
            .astype(BF16)
            .reshape(4, tokens, quarter)
            for piece in hid_y
        ]
    )
    y_place = lax.axis_index("y")
    partial = jnp.stack(
        [
            lax.dynamic_index_in_dim(partial, (c - y_place) & 3, 0, keepdims=False)
            for c in range(4)
        ],
        axis=1,
    )
    up, down = ring_step(*after((up, down), partial), "z")
    ring_pieces += [up, down]
    arrived = exchange(partial.reshape(16, tokens, quarter), ("x", "y"))
    projected = jnp.sum(arrived.astype(F32).reshape(4, 4, tokens, quarter), axis=0)
    mixed = pooled.astype(F32) + jnp.moveaxis(projected, 0, 1).reshape(tokens, D)
    length = jnp.sqrt(jnp.sum(mixed * mixed, axis=1, keepdims=True) + EPSILON)
    unit = mixed / length
    images = unit.astype(BF16)
    half = texts_y.shape[0] // 2
    up, down = after((up, down), images)
    ring_pieces += ring_step(up[:half], down[half:], "z")
    image_rows = joined([images] + [shift(images, x=s) for s in (1, 2, 3)])
    texts_own = jnp.concatenate(ring_pieces[:-2] + after(ring_pieces[-2:], image_rows))
    texts_other = shift(texts_own, k=1)
    part_a, loss_a = pair_tiles(scalars, image_rows, texts_own, None, tokens, batch_total)
    part, part_sent, loss_b = pair_tiles(
        scalars, image_rows, texts_other, part_a, tokens, batch_total
    )
    unit_grad = part[:tokens] + sum(
        shift(part_sent[s * tokens : (s + 1) * tokens], x=-s).astype(F32) for s in (1, 2, 3)
    )
    mixed_grad = (
        (unit_grad - unit * jnp.sum(unit * unit_grad, axis=1, keepdims=True)) / length
    ).astype(BF16)

    quarters = jnp.moveaxis(mixed_grad.reshape(tokens, 4, quarter), 1, 0)
    grad_rows = exchange(
        jnp.broadcast_to(quarters[None], (4, 4, tokens, quarter)).reshape(16, tokens, quarter),
        ("x", "y"),
    ).reshape(4, 4, tokens, quarter)
    grad_by_y = jnp.moveaxis(grad_rows, 1, 0).reshape(4, 4 * tokens, quarter)
    both = F32(0.0)
    for s in range(4):
        part = lax.dynamic_index_in_dim(grad_by_y, (y_place + s) & 3, 0, keepdims=False)
        both = both + lax.dot_general(
            part, hid_y[s], (((0,), (0,)), ((), ())), preferred_element_type=F32
        )
    low, high = both[:, :slice_ff], both[:, slice_ff:]
    chip_grad = jnp.where(first_core, low, high) + shift(jnp.where(first_core, high, low), k=1)
    arrived_grad = exchange(chip_grad.astype(BF16).reshape(8, D // 32, slice_ff), "z")
    gradient = jnp.sum(arrived_grad.astype(F32), axis=0)

    squared = gradient * gradient + FLOOR_VALUE
    row_message = jnp.concatenate([jnp.sum(squared, axis=1), jnp.sum(loss_a + loss_b).reshape(1)])
    row_total = jnp.sum(everywhere(row_message[None], ROW), axis=(0, 1))
    loss_row = row_total[-1]
    new_row = DECAY_RATE * row_moment + (1.0 - DECAY_RATE) * row_total[:-1] / FF
    scaled = jnp.sum(gradient * gradient / new_row[:, None], axis=0)
    col_message = jnp.concatenate(
        [jnp.sum(squared, axis=0), scaled, loss_row.reshape(1)]
    ).reshape(1, 2 * slice_ff + 1)
    col_total = jnp.sum(everywhere(col_message, COL), axis=(0, 1))
    new_col = DECAY_RATE * col_moment + (1.0 - DECAY_RATE) * col_total[:slice_ff] / D
    loss = col_total[-1] / batch_total
    ours = jnp.sum(col_total[slice_ff:-1] / new_col)
    update_total = jnp.sum(everywhere(jnp.full((1, 128), ours), ROW), axis=(0, 1))[0]
    update_rms = jnp.sqrt(update_total / (D * FF))
    raw_update = gradient / jnp.sqrt(new_row[:, None] * new_col[None, :])
    update = raw_update / jnp.maximum(1.0, update_rms / CLIP_LEVEL)
    return (update, new_row, new_col, loss)


def solution(mesh):
    finer = Mesh(mesh.devices.reshape(4, 2, 4, 8), AXES)
    return jax.shard_map(
        step,
        mesh=finer,
        in_specs=(
            P(AXES, None),
            P(AXES, None),
            P(AXES, None),
            P(COL, ROW),
            P(COL),
            P(ROW),
            P(),
            P(),
        ),
        out_specs=(P(COL, ROW), P(COL), P(ROW), P()),
        check_vma=False,
    )
```

```python
import functools
import itertools

import jax
import jax.numpy as jnp
from jax import lax
from jax.experimental import pallas as pl
from jax.experimental.pallas import tpu as pltpu
from jax.sharding import Mesh
from jax.sharding import PartitionSpec as P


D = 1152
FF = 4304
AXES = ("x", "k", "y", "z")
SIZES = {"x": 4, "k": 2, "y": 4, "z": 8}
ROW = ("x", "k")
COL = ("y", "z")
EPSILON = 1e-06
DECAY_RATE = 0.8
CLIP_LEVEL = 1.0
FLOOR_VALUE = 1e-30
BF16 = jnp.bfloat16
F32 = jnp.float32


def shift(value, **by):
    names = tuple(a for a in AXES if a in by)
    sizes = [SIZES[a] for a in names]

    def linear(place):
        index = 0
        for p, n in zip(place, sizes):
            index = index * n + p
        return index

    pairs = [
        (linear(p), linear([(c + by[a]) % SIZES[a] for c, a in zip(p, names)]))
        for p in itertools.product(*[range(n) for n in sizes])
    ]
    return lax.ppermute(value, names, pairs)


def exchange(pieces, axes):
    return lax.all_to_all(pieces, axes, split_axis=0, concat_axis=0, tiled=True)


def everywhere(array, axes):
    return exchange(jnp.broadcast_to(array, (lax.axis_size(axes), *array.shape)), axes)


def after(values, *others):
    return lax.optimization_barrier((values, others))[0]


def ring_step(up, down, axis):
    return shift(up, **{axis: 1}), shift(down, **{axis: -1})


def joined(pieces):
    rows = sum(p.shape[0] for p in pieces)
    whole = jnp.zeros((rows, *pieces[0].shape[1:]), pieces[0].dtype)
    at = 0
    for piece in pieces:
        whole = lax.dynamic_update_slice_in_dim(whole, piece, at, 0)
        at += piece.shape[0]
    return whole


def pair_kernel(scalars, images, texts, *refs, first, tokens, batch_total, block):
    if first:
        part, loss, kept = refs
        part[...] = jnp.zeros(part.shape, F32)
    else:
        before, part, sent, loss, kept = refs
        part[...] = before[...]
    loss[...] = jnp.zeros(loss.shape, F32)
    count = texts.shape[0] // block

    def block_of(at):
        return texts[pl.ds(pl.multiple_of(at * block, block), block), :]

    def logits_of(at):
        return (
            scalars[0]
            * lax.dot_general(
                images[...], block_of(at), (((1,), (1,)), ((), ())), preferred_element_type=F32
            )
            + scalars[1]
        )

    kept[0] = logits_of(0)

    def one(at, _):
        logits = kept[at & 1]
        kept[(at + 1) & 1] = logits_of(jnp.minimum(at + 1, count - 1))
        if first:
            rows = lax.broadcasted_iota(jnp.int32, logits.shape, 0)
            cols = lax.broadcasted_iota(jnp.int32, logits.shape, 1) + at * block
            positive = (rows == cols) & (rows < tokens)
            logits = jnp.where(positive, -logits, logits)
        small = jnp.exp(-jnp.abs(logits))
        base = 1.0 + small
        inverse = 1.0 / base
        slope = jnp.where(logits >= 0, inverse, small * inverse) / batch_total
        if first:
            slope = jnp.where(positive, -slope, slope)
        part[...] += jnp.dot(
            slope.astype(BF16), block_of(at), preferred_element_type=F32
        )
        softplus = jnp.maximum(logits, 0.0) + (
            jnp.log(base) + (small - (base - 1.0)) * inverse
        )
        loss[...] += jnp.sum(softplus, axis=0, keepdims=True)
        return 0

    lax.fori_loop(0, count, one, 0, unroll=2)
    if not first:
        scaled = scalars[0] * part[...]
        part[...] = scaled
        sent[...] = scaled.astype(BF16)


def pair_tiles(scalars, images, texts, before, tokens, batch_total):
    first = before is None
    count, width = images.shape
    block = 512
    outs = [jax.ShapeDtypeStruct((count, width), F32)]
    if not first:
        outs.append(jax.ShapeDtypeStruct((count, width), BF16))
    outs.append(jax.ShapeDtypeStruct((1, block), F32))
    pairs = count * texts.shape[0]
    return pl.pallas_call(
        functools.partial(
            pair_kernel, first=first, tokens=tokens, batch_total=batch_total, block=block
        ),
        in_specs=[pl.BlockSpec(memory_space=pltpu.SMEM)]
        + [pl.BlockSpec(memory_space=pltpu.VMEM)] * (2 if first else 3),
        out_shape=outs,
        scratch_shapes=[pltpu.VMEM((2, count, block), F32)],
        cost_estimate=pl.CostEstimate(
            flops=4 * pairs * width, bytes_accessed=2 * texts.size, transcendentals=3 * pairs
        ),
    )(scalars, images, texts, *([] if first else [before]))


def step(pooled, hidden, text, weight, row_moment, col_moment, log_scale, bias):
    tokens = pooled.shape[0]
    batch_total = tokens * 256
    slice_ff = weight.shape[1]
    k_place = lax.axis_index("k")

    first_core = k_place == 0
    quarter = D // 4
    x_place = lax.axis_index("x")
    hidden_by_x = jnp.moveaxis(hidden.reshape(tokens, 4, 2 * slice_ff), 1, 0)
    hidden_x = jnp.zeros((4, tokens, 2 * slice_ff), BF16)
    for s in range(4):
        piece = lax.dynamic_index_in_dim(hidden_by_x, (x_place + s) & 3, 0, keepdims=True)
        if s > 0:
            piece = shift(piece, x=s)
        hidden_x = lax.dynamic_update_index_in_dim(hidden_x, piece, (x_place - s) & 3, 0)
    hidden_x = hidden_x.reshape(4 * tokens, 2 * slice_ff)
    hid_y = [hidden_x] + [shift(hidden_x, y=-s) for s in (1, 2, 3)]

    text_float = text.astype(F32)
    text_units = (
        text_float / jnp.sqrt(jnp.sum(text_float * text_float, axis=1, keepdims=True) + EPSILON)
    ).astype(BF16)
    texts_y = joined([text_units] + [shift(text_units, k=1, y=s) for s in (1, 2, 3)])
    up, down = ring_step(texts_y, texts_y, "z")
    ring_pieces = [texts_y, up, down]
    scalars = jnp.stack([jnp.exp(log_scale), bias])
    weight_own = everywhere(after(weight.astype(BF16), hidden_x), "z")
    weight_own = after(weight_own.reshape(quarter, slice_ff), scalars)
    weight_other = after(shift(weight_own, k=1), up, down)
    up, down = ring_step(up, down, "z")
    ring_pieces += [up, down]
    weight_x = jnp.concatenate(
        [
            jnp.where(first_core, weight_own, weight_other),
            jnp.where(first_core, weight_other, weight_own),
        ],
        axis=1,
    )
    y_place = lax.axis_index("y")
    partial = jnp.zeros((4, 4, tokens, quarter), BF16)
    for s, piece in enumerate(hid_y):
        product = lax.dot_general(
            piece, weight_x, (((1,), (1,)), ((), ())), preferred_element_type=F32
        ).astype(BF16)
        partial = lax.dynamic_update_slice_in_dim(
            partial, product.reshape(4, 1, tokens, quarter), (y_place + s) & 3, 1
        )
    up, down = ring_step(*after((up, down), partial), "z")
    ring_pieces += [up, down]
    arrived = exchange(partial.reshape(16, tokens, quarter), ("x", "y"))
    projected = jnp.sum(arrived.astype(F32).reshape(4, 4, tokens, quarter), axis=0)
    mixed = pooled.astype(F32) + jnp.moveaxis(projected, 0, 1).reshape(tokens, D)
    length = jnp.sqrt(jnp.sum(mixed * mixed, axis=1, keepdims=True) + EPSILON)
    unit = mixed / length
    images = unit.astype(BF16)
    half = texts_y.shape[0] // 2
    up, down = after((up, down), images)
    ring_pieces += ring_step(up[:half], down[half:], "z")
    image_rows = joined([images] + [shift(images, x=s) for s in (1, 2, 3)])
    texts_own = jnp.concatenate(ring_pieces[:-2] + after(ring_pieces[-2:], image_rows))
    texts_other = shift(texts_own, k=1)
    part_a, loss_a = pair_tiles(scalars, image_rows, texts_own, None, tokens, batch_total)
    part, part_sent, loss_b = pair_tiles(
        scalars, image_rows, texts_other, part_a, tokens, batch_total
    )
    unit_grad = part[:tokens] + sum(
        shift(part_sent[s * tokens : (s + 1) * tokens], x=-s).astype(F32) for s in (1, 2, 3)
    )
    mixed_grad = (
        (unit_grad - unit * jnp.sum(unit * unit_grad, axis=1, keepdims=True)) / length
    ).astype(BF16)

    quarters = jnp.moveaxis(mixed_grad.reshape(tokens, 4, quarter), 1, 0)
    grad_rows = exchange(
        jnp.broadcast_to(quarters[None], (4, 4, tokens, quarter)).reshape(16, tokens, quarter),
        ("x", "y"),
    ).reshape(4, 4, tokens, quarter)
    grad_by_y = jnp.moveaxis(grad_rows, 1, 0).reshape(4, 4 * tokens, quarter)
    both = F32(0.0)
    for s in range(4):
        part = lax.dynamic_index_in_dim(grad_by_y, (y_place + s) & 3, 0, keepdims=False)
        both = both + lax.dot_general(
            part, hid_y[s], (((0,), (0,)), ((), ())), preferred_element_type=F32
        )
    low, high = both[:, :slice_ff], both[:, slice_ff:]
    chip_grad = jnp.where(first_core, low, high) + shift(jnp.where(first_core, high, low), k=1)
    arrived_grad = exchange(chip_grad.astype(BF16).reshape(8, D // 32, slice_ff), "z")
    gradient = jnp.sum(arrived_grad.astype(F32), axis=0)

    squared = gradient * gradient + FLOOR_VALUE
    row_message = jnp.concatenate([jnp.sum(squared, axis=1), jnp.sum(loss_a + loss_b).reshape(1)])
    row_total = jnp.sum(everywhere(row_message[None], ROW), axis=(0, 1))
    loss_row = row_total[-1]
    new_row = DECAY_RATE * row_moment + (1.0 - DECAY_RATE) * row_total[:-1] / FF
    scaled = jnp.sum(gradient * gradient / new_row[:, None], axis=0)
    col_message = jnp.concatenate(
        [jnp.sum(squared, axis=0), scaled, loss_row.reshape(1)]
    ).reshape(1, 2 * slice_ff + 1)
    col_total = jnp.sum(everywhere(col_message, COL), axis=(0, 1))
    new_col = DECAY_RATE * col_moment + (1.0 - DECAY_RATE) * col_total[:slice_ff] / D
    loss = col_total[-1] / batch_total
    ours = jnp.sum(col_total[slice_ff:-1] / new_col)
    update_total = jnp.sum(everywhere(jnp.full((1, 128), ours), ROW), axis=(0, 1))[0]
    update_rms = jnp.sqrt(update_total / (D * FF))
    raw_update = gradient / jnp.sqrt(new_row[:, None] * new_col[None, :])
    update = raw_update / jnp.maximum(1.0, update_rms / CLIP_LEVEL)
    return (update, new_row, new_col, loss)


def solution(mesh):
    finer = Mesh(mesh.devices.reshape(4, 2, 4, 8), AXES)
    return jax.shard_map(
        step,
        mesh=finer,
        in_specs=(
            P(AXES, None),
            P(AXES, None),
            P(AXES, None),
            P(COL, ROW),
            P(COL),
            P(ROW),
            P(),
            P(),
        ),
        out_specs=(P(COL, ROW), P(COL), P(ROW), P()),
        check_vma=False,
    )
```

```python
import functools
import itertools

import jax
import jax.numpy as jnp
from jax import lax
from jax.experimental import pallas as pl
from jax.experimental.pallas import tpu as pltpu
from jax.sharding import Mesh
from jax.sharding import PartitionSpec as P


D = 1152
FF = 4304
AXES = ("x", "k", "y", "z")
SIZES = {"x": 4, "k": 2, "y": 4, "z": 8}
ROW = ("x", "k")
COL = ("y", "z")
EPSILON = 1e-06
DECAY_RATE = 0.8
CLIP_LEVEL = 1.0
FLOOR_VALUE = 1e-30
BF16 = jnp.bfloat16
F32 = jnp.float32


def shift(value, **by):
    names = tuple(a for a in AXES if a in by)
    sizes = [SIZES[a] for a in names]

    def linear(place):
        index = 0
        for p, n in zip(place, sizes):
            index = index * n + p
        return index

    pairs = [
        (linear(p), linear([(c + by[a]) % SIZES[a] for c, a in zip(p, names)]))
        for p in itertools.product(*[range(n) for n in sizes])
    ]
    return lax.ppermute(value, names, pairs)


def exchange(pieces, axes):
    return lax.all_to_all(pieces, axes, split_axis=0, concat_axis=0, tiled=True)


def everywhere(array, axes):
    return exchange(jnp.broadcast_to(array, (lax.axis_size(axes), *array.shape)), axes)


def after(values, *others):
    return lax.optimization_barrier((values, others))[0]


def ring_step(up, down, axis):
    return shift(up, **{axis: 1}), shift(down, **{axis: -1})


def joined(pieces):
    rows = sum(p.shape[0] for p in pieces)
    whole = jnp.zeros((rows, *pieces[0].shape[1:]), pieces[0].dtype)
    at = 0
    for piece in pieces:
        whole = lax.dynamic_update_slice_in_dim(whole, piece, at, 0)
        at += piece.shape[0]
    return whole


def pair_kernel(scalars, images, texts, *refs, first, tokens, batch_total, block):
    if first:
        part, loss, kept = refs
        part[...] = jnp.zeros(part.shape, F32)
    else:
        before, part, sent, loss, kept = refs
        part[...] = before[...]
    loss[...] = jnp.zeros(loss.shape, F32)
    count = texts.shape[0] // block

    def block_of(at):
        return texts[pl.ds(pl.multiple_of(at * block, block), block), :]

    def logits_of(at):
        return (
            scalars[0]
            * lax.dot_general(
                images[...], block_of(at), (((1,), (1,)), ((), ())), preferred_element_type=F32
            )
            + scalars[1]
        )

    kept[0] = logits_of(0)

    def one(at, _):
        logits = kept[at & 1]
        kept[(at + 1) & 1] = logits_of(jnp.minimum(at + 1, count - 1))
        if first:
            rows = lax.broadcasted_iota(jnp.int32, logits.shape, 0)
            cols = lax.broadcasted_iota(jnp.int32, logits.shape, 1) + at * block
            positive = (rows == cols) & (rows < tokens)
            logits = jnp.where(positive, -logits, logits)
        small = jnp.exp(-jnp.abs(logits))
        base = 1.0 + small
        inverse = 1.0 / base
        slope = jnp.where(logits >= 0, inverse, small * inverse) / batch_total
        if first:
            slope = jnp.where(positive, -slope, slope)
        part[...] += jnp.dot(
            slope.astype(BF16), block_of(at), preferred_element_type=F32
        )
        softplus = jnp.maximum(logits, 0.0) + (
            jnp.log(base) + (small - (base - 1.0)) * inverse
        )
        loss[...] += jnp.sum(softplus, axis=0, keepdims=True)
        return 0

    lax.fori_loop(0, count, one, 0, unroll=2)
    if not first:
        scaled = scalars[0] * part[...]
        part[...] = scaled
        sent[...] = scaled.astype(BF16)


def pair_tiles(scalars, images, texts, before, tokens, batch_total):
    first = before is None
    count, width = images.shape
    block = 512
    outs = [jax.ShapeDtypeStruct((count, width), F32)]
    if not first:
        outs.append(jax.ShapeDtypeStruct((count, width), BF16))
    outs.append(jax.ShapeDtypeStruct((1, block), F32))
    pairs = count * texts.shape[0]
    return pl.pallas_call(
        functools.partial(
            pair_kernel, first=first, tokens=tokens, batch_total=batch_total, block=block
        ),
        in_specs=[pl.BlockSpec(memory_space=pltpu.SMEM)]
        + [pl.BlockSpec(memory_space=pltpu.VMEM)] * (2 if first else 3),
        out_shape=outs,
        scratch_shapes=[pltpu.VMEM((2, count, block), F32)],
        cost_estimate=pl.CostEstimate(
            flops=4 * pairs * width, bytes_accessed=2 * texts.size, transcendentals=3 * pairs
        ),
    )(scalars, images, texts, *([] if first else [before]))


def step(pooled, hidden, text, weight, row_moment, col_moment, log_scale, bias):
    tokens = pooled.shape[0]
    batch_total = tokens * 256
    slice_ff = weight.shape[1]
    k_place = lax.axis_index("k")

    first_core = k_place == 0
    quarter = D // 4
    x_place = lax.axis_index("x")
    hidden_by_x = jnp.moveaxis(hidden.reshape(tokens, 4, 2 * slice_ff), 1, 0)
    hidden_x = jnp.zeros((4, tokens, 2 * slice_ff), BF16)
    for s in range(4):
        piece = lax.dynamic_index_in_dim(hidden_by_x, (x_place + s) & 3, 0, keepdims=True)
        if s > 0:
            piece = shift(piece, x=s)
        hidden_x = lax.dynamic_update_index_in_dim(hidden_x, piece, (x_place - s) & 3, 0)
    hidden_x = hidden_x.reshape(4 * tokens, 2 * slice_ff)
    hid_y = [hidden_x] + [shift(hidden_x, y=-s) for s in (1, 2, 3)]

    text_float = text.astype(F32)
    text_units = (
        text_float / jnp.sqrt(jnp.sum(text_float * text_float, axis=1, keepdims=True) + EPSILON)
    ).astype(BF16)
    texts_y = joined([text_units] + [shift(text_units, k=1, y=s) for s in (1, 2, 3)])
    up, down = ring_step(texts_y, texts_y, "z")
    ring_pieces = [texts_y, up, down]
    scalars = jnp.stack([jnp.exp(log_scale), bias])
    weight_own = everywhere(after(weight.astype(BF16), hidden_x), "z")
    weight_own = weight_own.reshape(quarter, slice_ff)
    weight_own = after(weight_own, scalars)
    weight_other = shift(weight_own, k=1)
    weight_x = jnp.concatenate(
        [
            jnp.where(first_core, weight_own, weight_other),
            jnp.where(first_core, weight_other, weight_own),
        ],
        axis=1,
    )
    up, down = ring_step(up, down, "z")
    ring_pieces += [up, down]
    y_place = lax.axis_index("y")
    partial = jnp.zeros((4, 4, tokens, quarter), BF16)
    for s, piece in enumerate(hid_y):
        product = lax.dot_general(
            piece, weight_x, (((1,), (1,)), ((), ())), preferred_element_type=F32
        ).astype(BF16)
        partial = lax.dynamic_update_slice_in_dim(
            partial, product.reshape(4, 1, tokens, quarter), (y_place + s) & 3, 1
        )
    up, down = ring_step(*after((up, down), partial), "z")
    ring_pieces += [up, down]
    arrived = exchange(partial.reshape(16, tokens, quarter), ("x", "y"))
    projected = jnp.sum(arrived.astype(F32).reshape(4, 4, tokens, quarter), axis=0)
    mixed = pooled.astype(F32) + jnp.moveaxis(projected, 0, 1).reshape(tokens, D)
    length = jnp.sqrt(jnp.sum(mixed * mixed, axis=1, keepdims=True) + EPSILON)
    unit = mixed / length
    images = unit.astype(BF16)
    half = texts_y.shape[0] // 2
    up, down = after((up, down), images)
    ring_pieces += ring_step(up[:half], down[half:], "z")
    image_rows = joined([images] + [shift(images, x=s) for s in (1, 2, 3)])
    texts_own = jnp.concatenate(ring_pieces[:-2] + after(ring_pieces[-2:], image_rows))
    texts_other = shift(texts_own, k=1)
    part_a, loss_a = pair_tiles(scalars, image_rows, texts_own, None, tokens, batch_total)
    part, part_sent, loss_b = pair_tiles(
        scalars, image_rows, texts_other, part_a, tokens, batch_total
    )
    unit_grad = part[:tokens] + sum(
        shift(part_sent[s * tokens : (s + 1) * tokens], x=-s).astype(F32) for s in (1, 2, 3)
    )
    mixed_grad = (
        (unit_grad - unit * jnp.sum(unit * unit_grad, axis=1, keepdims=True)) / length
    ).astype(BF16)

    quarters = jnp.moveaxis(mixed_grad.reshape(tokens, 4, quarter), 1, 0)
    grad_rows = exchange(
        jnp.broadcast_to(quarters[None], (4, 4, tokens, quarter)).reshape(16, tokens, quarter),
        ("x", "y"),
    ).reshape(4, 4, tokens, quarter)
    grad_by_y = jnp.moveaxis(grad_rows, 1, 0).reshape(4, 4 * tokens, quarter)
    both = F32(0.0)
    for s in range(4):
        part = lax.dynamic_index_in_dim(grad_by_y, (y_place + s) & 3, 0, keepdims=False)
        both = both + lax.dot_general(
            part, hid_y[s], (((0,), (0,)), ((), ())), preferred_element_type=F32
        )
    low, high = both[:, :slice_ff], both[:, slice_ff:]
    chip_grad = jnp.where(first_core, low, high) + shift(jnp.where(first_core, high, low), k=1)
    arrived_grad = exchange(chip_grad.astype(BF16).reshape(8, D // 32, slice_ff), "z")
    gradient = jnp.sum(arrived_grad.astype(F32), axis=0)

    squared = gradient * gradient + FLOOR_VALUE
    row_message = jnp.concatenate([jnp.sum(squared, axis=1), jnp.sum(loss_a + loss_b).reshape(1)])
    row_total = jnp.sum(everywhere(row_message[None], ROW), axis=(0, 1))
    loss_row = row_total[-1]
    new_row = DECAY_RATE * row_moment + (1.0 - DECAY_RATE) * row_total[:-1] / FF
    scaled = jnp.sum(gradient * gradient / new_row[:, None], axis=0)
    col_message = jnp.concatenate(
        [jnp.sum(squared, axis=0), scaled, loss_row.reshape(1)]
    ).reshape(1, 2 * slice_ff + 1)
    col_total = jnp.sum(everywhere(col_message, COL), axis=(0, 1))
    new_col = DECAY_RATE * col_moment + (1.0 - DECAY_RATE) * col_total[:slice_ff] / D
    loss = col_total[-1] / batch_total
    ours = jnp.sum(col_total[slice_ff:-1] / new_col)
    update_total = jnp.sum(everywhere(jnp.full((1, 128), ours), ROW), axis=(0, 1))[0]
    update_rms = jnp.sqrt(update_total / (D * FF))
    raw_update = gradient / jnp.sqrt(new_row[:, None] * new_col[None, :])
    update = raw_update / jnp.maximum(1.0, update_rms / CLIP_LEVEL)
    return (update, new_row, new_col, loss)


def solution(mesh):
    finer = Mesh(mesh.devices.reshape(4, 2, 4, 8), AXES)
    return jax.shard_map(
        step,
        mesh=finer,
        in_specs=(
            P(AXES, None),
            P(AXES, None),
            P(AXES, None),
            P(COL, ROW),
            P(COL),
            P(ROW),
            P(),
            P(),
        ),
        out_specs=(P(COL, ROW), P(COL), P(ROW), P()),
        check_vma=False,
    )
```
